128 devices in a mesh: chord: 8 (over y_lo, z), span: 16 (over x, y_hi, core).
Axes of the slice: x: 4, y: 4 (y_hi: 2, y_lo: 2; y = y_hi * 2 + y_lo), z: 4, core: 2. Of those that a mesh axis runs over, the one named last changes fastest.
Arguments:
- state: float32 [5, 125, 32, 32, 128], P(None, None, 'chord', 'span'), may hold values from -10 to 10
Outputs:
- residual: float32 [5, 125, 32, 32, 128], P(None, None, 'chord', 'span')
- viscosity: float32 [125, 32, 32, 128], P(None, 'chord', 'span')
The draws below stay inside these ranges and needn't reach their ends.
All inputs are finite; a program needn't handle non-finite values.
Results may differ from the reference program's by a relative error of at most 0.0001.
Values sent between devices are 32-bit elements; how exact they have to be, the bound alone decides.
No kernel may reach another device: no remote copies, remote signals or barrier semaphores. Data moves between devices by JAX's collectives and lax.ppermute only.
A program may use at most 128 MiB of HBM per device.

```python
import math
import jax
import jax.numpy as jnp
import numpy as np
from jax import lax

NVAR = 5
NPTS = 125
NORMAL_ELEMENTS = 128
CHORD_ELEMENTS = 32
SPAN_ELEMENTS = 32


def draw_state(key, part):
    element_lattice = (CHORD_ELEMENTS, SPAN_ELEMENTS, NORMAL_ELEMENTS)
    variable = jnp.arange(NVAR).reshape(NVAR, 1, 1, 1, 1)
    level_base = jax.random.normal(jax.random.fold_in(key, 1), (NVAR, 1) + element_lattice, jnp.float32)
    density_base = jax.random.uniform(jax.random.fold_in(key, 2), (NVAR, 1) + element_lattice, jnp.float32, 0.5, 1.5)
    base = jnp.where(variable == 0, density_base, level_base)
    log_amp = jax.random.uniform(jax.random.fold_in(key, 3), (NVAR, 1) + element_lattice, jnp.float32, math.log(0.001), math.log(1.0))
    noise = jax.random.normal(jax.random.fold_in(key, 4), (NVAR, NPTS) + element_lattice, jnp.float32)
    return jnp.clip(base + jnp.exp(log_amp) * noise, -10.0, 10.0)


def setup_inputs(seed: int = 0) -> dict:
    key_of = jax.random.split(jax.random.key(seed), 2)
    return {
        "state": draw_state(jax.random.fold_in(key_of[1], 71), 0),
    }


EPS_SCALE = 0.01
SENSOR_CENTRE = -3.0
SENSOR_WIDTH = 1.5
RATIO_FLOOR = 1e-06
ENERGY_EPS = 1e-06
GAUSS_NODES = [-0.906179845938664, -0.5384693101056831, 0.0, 0.5384693101056831, 0.906179845938664]
GAUSS_WEIGHTS = [0.2369268850561891, 0.4786286704993665, 0.5688888888888889, 0.4786286704993665, 0.2369268850561891]

def legendre_values(points):
    values = [np.ones(points.shape), np.array(points)]
    for order in range(1, 5):
        values.append(((2 * order + 1) * points * values[order] - order * values[order - 1]) / (order + 1))
    return values

def line_tables():
    line_nodes = np.array(GAUSS_NODES)
    quadrature_weights = np.array(GAUSS_WEIGHTS)
    barycentric = np.array([1.0 / np.prod([line_nodes[j] - line_nodes[k] for k in range(5) if k != j]) for j in range(5)])
    derivative = np.zeros((5, 5))
    for i in range(5):
        for j in range(5):
            if i != j:
                derivative[i, j] = barycentric[j] / barycentric[i] / (line_nodes[i] - line_nodes[j])
        derivative[i, i] = -np.sum(derivative[i])
    left_values = np.ones(5)
    right_values = np.ones(5)
    for j in range(5):
        for k in range(5):
            if k != j:
                left_values[j] *= (-1.0 - line_nodes[k]) / (line_nodes[j] - line_nodes[k])
                right_values[j] *= (1.0 - line_nodes[k]) / (line_nodes[j] - line_nodes[k])
    legendre = legendre_values(line_nodes)
    fourth_slope = 7.0 * legendre[3] + 3.0 * legendre[1]
    fifth_slope = 9.0 * legendre[4] + 5.0 * legendre[2] + legendre[0]
    left_corr = 0.5 * (fourth_slope - fifth_slope)
    right_corr = 0.5 * (fourth_slope + fifth_slope)
    modal = np.zeros((5, 5))
    for k in range(5):
        modal[k, :] = quadrature_weights * math.sqrt((2 * k + 1) / 2.0) * legendre[k]
    return (line_nodes, derivative, left_values, right_values, left_corr, right_corr, modal)

def along_axis(operator_matrix, axis):
    factors = [np.eye(5), np.eye(5), np.eye(5)]
    factors[axis] = operator_matrix
    return np.kron(np.kron(factors[0], factors[1]), factors[2])

def build_tables():
    line_nodes, derivative, left_values, right_values, left_corr, right_corr, modal = line_tables()
    operators = []
    for axis in range(3):
        group = (along_axis(derivative, axis), along_axis(left_values[None, :], axis), along_axis(right_values[None, :], axis), along_axis(left_corr[:, None], axis), along_axis(right_corr[:, None], axis))
        operators.append(tuple((jnp.asarray(entry, dtype=jnp.float32) for entry in group)))
    modal_3d = jnp.asarray(np.kron(np.kron(modal, modal), modal), dtype=jnp.float32)
    point_index = np.arange(125)
    high_np = np.where((point_index // 25 == 4) | (point_index // 5 % 5 == 4) | (point_index % 5 == 4), 1.0, 0.0)
    high_mask = jnp.asarray(high_np, dtype=jnp.float32)
    halves = [(1.0 - line_nodes) / 2.0, (1.0 + line_nodes) / 2.0]
    trilinear_np = np.zeros((125, 8))
    for corner in range(8):
        trilinear_np[:, corner] = np.kron(np.kron(halves[corner // 4], halves[corner // 2 % 2]), halves[corner % 2])
    trilinear = jnp.asarray(trilinear_np, dtype=jnp.float32)
    return (operators, modal_3d, high_mask, trilinear)

def single_points(operator_matrix, field):
    return jnp.einsum('qp,pxyz->qxyz', operator_matrix, field, precision=lax.Precision.HIGHEST)

def sensor_viscosity(density, modal_3d, high_mask):
    coeffs = single_points(modal_3d, density)
    energy = coeffs * coeffs
    high_part = lax.optimization_barrier(jnp.sum(energy * high_mask[:, None, None, None], axis=0))
    total = lax.optimization_barrier(jnp.sum(energy, axis=0)) + ENERGY_EPS
    level = jnp.log10(jnp.maximum(high_part / total, RATIO_FLOOR))
    ramp = jnp.clip((level - SENSOR_CENTRE) / SENSOR_WIDTH, -1.0, 1.0)
    return EPS_SCALE * 0.5 * (1.0 + jnp.sin(0.5 * math.pi * ramp))

def boundary_masks(length, dim, rank, is_first, is_last):
    shape = [1] * rank
    shape[dim] = length
    place = lax.broadcasted_iota(jnp.int32, tuple(shape), dim)
    lower_open = jnp.logical_or(place > 0, jnp.logical_not(is_first))
    upper_open = jnp.logical_or(place < length - 1, jnp.logical_not(is_last))
    return (lower_open.astype(jnp.float32), upper_open.astype(jnp.float32))

def variable_residual(field, viscosity, operators):
    total = jnp.zeros_like(field)
    for axis in range(3):
        derivative, to_left, to_right, lift_left, lift_right = operators[axis]
        dim = axis + 1
        closed = axis != 1
        lower_open, upper_open = boundary_masks(field.shape[dim], dim, 4, closed, closed)
        left_tr = single_points(to_left, field)
        right_tr = single_points(to_right, field)
        prev_right = jnp.roll(right_tr, 1, axis=dim)
        following_left = jnp.roll(left_tr, -1, axis=dim)
        gradient = single_points(derivative, field) + single_points(lift_left, 0.5 * (prev_right - left_tr) * lower_open) + single_points(lift_right, 0.5 * (following_left - right_tr) * upper_open)
        flux = viscosity * gradient
        flux_left = single_points(to_left, flux)
        flux_right = single_points(to_right, flux)
        flux_prev = jnp.roll(flux_right, 1, axis=dim)
        flux_next = jnp.roll(flux_left, -1, axis=dim)
        total = total + single_points(derivative, flux) + single_points(lift_left, 0.5 * (flux_prev + flux_left) * lower_open - flux_left) + single_points(lift_right, 0.5 * (flux_next + flux_right) * upper_open - flux_right)
    return total

def reference(state):
    operators, modal_3d, high_mask, trilinear = build_tables()
    element_eps = sensor_viscosity(state[0], modal_3d, high_mask)
    padded = jnp.pad(element_eps, ((1, 1), (0, 0), (1, 1)))
    along_chord = jnp.maximum(padded[:-1], padded[1:])
    along_span = jnp.maximum(along_chord, jnp.roll(along_chord, 1, axis=1))
    vertex = jnp.maximum(along_span[:, :, :-1], along_span[:, :, 1:])
    shifted = jnp.roll(vertex, -1, axis=1)
    chord_count = element_eps.shape[0]
    normal_count = element_eps.shape[2]
    corner_list = []
    for corner in range(8):
        step_x = corner // 4
        step_y = corner // 2 % 2
        step_z = corner % 2
        source = shifted if step_y == 1 else vertex
        corner_list.append(source[step_x:step_x + chord_count, :, step_z:step_z + normal_count])
    corners = jnp.stack(corner_list, axis=0)
    viscosity = jnp.einsum('qc,cxyz->qxyz', trilinear, corners, precision=lax.Precision.HIGHEST)

    def one_variable(field):
        return variable_residual(field, viscosity, operators)
    residual = lax.map(one_variable, state)
    return (residual, viscosity)
```

```python
import functools
import math

import jax
import jax.numpy as jnp
import numpy as np
from jax import lax
from jax.experimental import pallas as pl
from jax.experimental.pallas import tpu as pltpu
from jax.sharding import PartitionSpec as P

EPS_SCALE = 0.01
SENSOR_CENTRE = -3.0
SENSOR_WIDTH = 1.5
RATIO_FLOOR = 1e-06
ENERGY_EPS = 1e-06
GAUSS_NODES = [-0.906179845938664, -0.5384693101056831, 0.0, 0.5384693101056831, 0.906179845938664]
GAUSS_WEIGHTS = [
    0.2369268850561891,
    0.4786286704993665,
    0.5688888888888889,
    0.4786286704993665,
    0.2369268850561891,
]


def legendre_values(points):
    values = [np.ones(points.shape), np.array(points)]
    for order in range(1, 5):
        values.append(
            ((2 * order + 1) * points * values[order] - order * values[order - 1]) / (order + 1)
        )
    return values


def line_tables():
    line_nodes = np.array(GAUSS_NODES)
    quadrature_weights = np.array(GAUSS_WEIGHTS)
    barycentric = np.array(
        [
            1.0 / np.prod([line_nodes[j] - line_nodes[k] for k in range(5) if k != j])
            for j in range(5)
        ]
    )
    derivative = np.zeros((5, 5))
    for i in range(5):
        for j in range(5):
            if i != j:
                derivative[i, j] = barycentric[j] / barycentric[i] / (line_nodes[i] - line_nodes[j])
        derivative[i, i] = -np.sum(derivative[i])
    left_values = np.ones(5)
    right_values = np.ones(5)
    for j in range(5):
        for k in range(5):
            if k != j:
                left_values[j] *= (-1.0 - line_nodes[k]) / (line_nodes[j] - line_nodes[k])
                right_values[j] *= (1.0 - line_nodes[k]) / (line_nodes[j] - line_nodes[k])
    legendre = legendre_values(line_nodes)
    fourth_slope = 7.0 * legendre[3] + 3.0 * legendre[1]
    fifth_slope = 9.0 * legendre[4] + 5.0 * legendre[2] + legendre[0]
    modal = np.zeros((5, 5))
    for k in range(5):
        modal[k, :] = quadrature_weights * math.sqrt((2 * k + 1) / 2.0) * legendre[k]
    return (line_nodes, derivative, left_values, right_values, fourth_slope, fifth_slope, modal)


NODES, DERIV, LEFT, RIGHT, SLOPE4, SLOPE5, MODAL = line_tables()
CORR_L = 0.5 * (SLOPE4 - SLOPE5)
CORR_R = 0.5 * (SLOPE4 + SLOPE5)
OWN = DERIV - 0.5 * (np.outer(CORR_L, LEFT) + np.outer(CORR_R, RIGHT))
ROWS, LANES = 8, 128
NV, NF = 5, 25
SPAN_V, CHORD_V = 13, 7
SPAN_N, CHORD_N = NV * SPAN_V, NV * CHORD_V


def mul(scale, x):
    return float(scale) * x


def even_odd(x):
    return (x[0] + x[4], x[1] + x[3], x[0] - x[4], x[1] - x[3], x[2])


def traces(parts):
    e0, e1, o0, o1, c = parts
    even = (
        mul(0.5 * (LEFT[0] + LEFT[4]), e0) + mul(0.5 * (LEFT[1] + LEFT[3]), e1) + mul(LEFT[2], c)
    )
    odd = mul(0.5 * (LEFT[0] - LEFT[4]), o0) + mul(0.5 * (LEFT[1] - LEFT[3]), o1)
    return (even + odd, even - odd)


def slope(parts, total, diff):
    e0, e1, o0, o1, c = parts
    even, odd = [], []
    for i in range(3):
        even.append(
            mul(0.5 * (OWN[i, 0] - OWN[i, 4]), o0)
            + mul(0.5 * (OWN[i, 1] - OWN[i, 3]), o1)
            + mul(0.25 * SLOPE5[i], diff)
        )
    for i in range(2):
        odd.append(
            mul(0.5 * (OWN[i, 0] + OWN[i, 4]), e0)
            + mul(0.5 * (OWN[i, 1] + OWN[i, 3]), e1)
            + (mul(OWN[i, 2], c) + mul(0.25 * SLOPE4[i], total))
        )
    return [
        even[0] + odd[0],
        even[1] + odd[1],
        even[2],
        even[1] - odd[1],
        even[0] - odd[0],
    ]


def modal_line(x):
    e0, e1, o0, o1, c = even_odd(x)
    out = []
    for k in range(5):
        if k % 2 == 0:
            out.append(mul(MODAL[k, 0], e0) + mul(MODAL[k, 1], e1) + mul(MODAL[k, 2], c))
        else:
            out.append(mul(MODAL[k, 0], o0) + mul(MODAL[k, 1], o1))
    return out


def line_points(axis, f):
    a, b = f // 5, f % 5
    if axis == 0:
        return [25 * k + 5 * a + b for k in range(5)]
    if axis == 1:
        return [25 * a + 5 * k + b for k in range(5)]
    return [25 * a + 5 * b + k for k in range(5)]


def row_ids():
    rows = lax.broadcasted_iota(jnp.int32, (ROWS, LANES), 0)
    return (rows // 2, rows % 2)


def lane_ids():
    return lax.broadcasted_iota(jnp.int32, (ROWS, LANES), 1)


def up_rows(x, n):
    n = n % ROWS
    return x if n == 0 else pltpu.roll(x, n, 0)


def splat_flag(flag):
    return jnp.full((ROWS, LANES), flag.astype(jnp.int32), jnp.int32) > 0


def even_span():
    return splat_flag(lax.axis_index("span") % 2 == 0)


def even_chord():
    return splat_flag(lax.axis_index("chord") % 2 == 0)


def pack_span(out_of, is_low, even, first_ref, second_ref, base):
    for m in range(SPAN_V):
        f0 = out_of(2 * m)
        f1 = out_of(2 * m + 1) if 2 * m + 1 < NF else f0
        up = jnp.where(is_low, up_rows(f0, -1), f1)
        down = jnp.where(is_low, f0, up_rows(f1, 1))
        first_ref[base + m] = jnp.where(even, up, down)
        second_ref[base + m] = jnp.where(even, down, up)


def pack_chord(out_of, i, even, first_ref, second_ref, base):
    for m in range(CHORD_V):
        up = down = None
        for q in range(4):
            f = 4 * m + q
            if f >= NF:
                continue
            trace = out_of(f)
            u, d = up_rows(trace, 2 * q - 6), up_rows(trace, 2 * q)
            up = u if up is None else jnp.where(i == q, u, up)
            down = d if down is None else jnp.where(i == q, d, down)
        first_ref[base + m] = jnp.where(even, up, down)
        second_ref[base + m] = jnp.where(even, down, up)


def open_span(below, above, q, is_low):
    if q == 0:
        return jnp.where(is_low, below, up_rows(above, 1))
    return jnp.where(is_low, up_rows(below, -1), above)


def open_chord(below, above, q, i):
    return jnp.where(i == 0, up_rows(below, -2 * q), up_rows(above, 6 - 2 * q))


def leave_kernel(state, so, se, co, ce, eps_ref, work):
    i, j = row_ids()
    is_low, first_row = j == 0, i == 0
    es, ec = even_span(), even_chord()

    def one(v, carry):
        def leaving(axis, mask, f):
            left, right = traces(even_odd([state[v, p] for p in line_points(axis, f)]))
            return jnp.where(mask, left, right)

        pack_span(functools.partial(leaving, 1, is_low), is_low, es, se, so, v * SPAN_V)
        pack_chord(functools.partial(leaving, 0, first_row), i, ec, ce, co, v * CHORD_V)
        return carry

    lax.fori_loop(0, NV, one, 0)
    for axis in range(2):
        source = state.at[0] if axis == 0 else work
        for f in range(NF):
            points = line_points(axis, f)
            for p, value in zip(points, modal_line([source[p] for p in points])):
                work[p] = value
    low_sums, high_sums = [], []
    for f in range(NF):
        a, b = f // 5, f % 5
        low, high = None, None
        for k, value in enumerate(modal_line([work[p] for p in line_points(2, f)])):
            square = value * value
            if a == 4 or b == 4 or k == 4:
                high = square if high is None else high + square
            else:
                low = square if low is None else low + square
        if low is not None:
            low_sums.append(low)
        high_sums.append(high)

    def tree(values):
        while len(values) > 1:
            values = [
                values[n] + values[n + 1] if n + 1 < len(values) else values[n]
                for n in range(0, len(values), 2)
            ]
        return values[0]

    high_part = tree(high_sums)
    total = (tree(low_sums) + high_part) + ENERGY_EPS
    level = jnp.log(jnp.maximum(high_part / total, RATIO_FLOOR)) * (1.0 / math.log(10.0))
    ramp = jnp.clip((level - SENSOR_CENTRE) / SENSOR_WIDTH, -1.0, 1.0)
    eps = EPS_SCALE * 0.5 * (1.0 + jnp.sin(0.5 * math.pi * ramp))
    eps_ref[...] = eps
    for ref, at in ((so, SPAN_N), (se, SPAN_N), (co, CHORD_N), (ce, CHORD_N)):
        ref[at] = eps


def corner_kernel(rce, rco, cor):
    ec = even_chord()
    first, second = rce[CHORD_N], rco[CHORD_N]
    cor[0] = jnp.where(ec, second, first)
    cor[1] = jnp.where(ec, first, second)


def neighbours_chord(left, right, sign, i):
    first = (lax.axis_index("chord") == 0).astype(jnp.float32) * sign
    last = (lax.axis_index("chord") == lax.axis_size("chord") - 1).astype(jnp.float32) * sign
    before = jnp.where(i == 0, left * first, up_rows(right, 2))
    after = jnp.where(i == 3, right * last, up_rows(left, -2))
    return (before + after, after - before)


def neighbours_span(left, right, is_low, sign_row):
    inner = jnp.where(is_low, up_rows(left, -1), up_rows(right, 1))
    return (inner, inner * sign_row)


def neighbours_normal(left, right, sign, lane):
    before = jnp.where(lane == 0, mul(sign, left), pltpu.roll(right, 1, 1))
    after = jnp.where(lane == LANES - 1, mul(sign, right), pltpu.roll(left, LANES - 1, 1))
    return (before + after, after - before)


def gradient_kernel(state, gc, gs, gn, total_ref, diff_ref):
    i, j = row_ids()
    lane = lane_ids()
    is_low = j == 0
    sign_row = jnp.where(is_low, 1.0, -1.0)

    def one(v, carry):
        def lines(axis, f):
            return even_odd([state[v, p] for p in line_points(axis, f)])

        for f in range(NF):
            left, right = traces(lines(2, f))
            total_ref[f], diff_ref[f] = neighbours_normal(left, right, 1.0, lane)
        for axis, ref in ((0, gc), (1, gs), (2, gn)):
            for f in range(NF):
                parts = lines(axis, f)
                if axis == 2:
                    total, diff = total_ref[f], diff_ref[f]
                else:
                    left, right = traces(parts)
                    if axis == 0:
                        total, diff = neighbours_chord(left, right, 1.0, i)
                    else:
                        total, diff = neighbours_span(left, right, is_low, sign_row)
                for p, value in zip(line_points(axis, f), slope(parts, total, diff)):
                    ref[v, p] = value
        return carry

    lax.fori_loop(0, NV, one, 0)


def viscosity_into(visc, own, below, above, before, after, cb, ca):
    i, j = row_ids()
    lane = lane_ids()
    is_low = j == 0

    def chord_pair(mid, low, high):
        under = up_rows(jnp.where(i == 3, low, mid), 2)
        over = up_rows(jnp.where(i == 0, high, mid), -2)
        return (jnp.maximum(mid, under), jnp.maximum(mid, over))

    mids = chord_pair(own, below, above)
    befores = chord_pair(before, cb[0], cb[1])
    afters = chord_pair(after, ca[0], ca[1])
    corners = {}
    for x in range(2):
        mid, low, high = mids[x], befores[x], afters[x]
        under = jnp.where(is_low, up_rows(low, -1), up_rows(mid, 1))
        over = jnp.where(is_low, up_rows(mid, -1), up_rows(high, 1))
        for y, value in enumerate((jnp.maximum(mid, under), jnp.maximum(mid, over))):
            low_z = jnp.where(lane == 0, value, pltpu.roll(value, 1, 1))
            high_z = jnp.where(lane == LANES - 1, value, pltpu.roll(value, LANES - 1, 1))
            corners[x, y, 0] = jnp.maximum(value, low_z)
            corners[x, y, 1] = jnp.maximum(value, high_z)
    halves = [((1.0 - x) / 2.0, (1.0 + x) / 2.0) for x in NODES]
    for a in range(5):
        plane = {
            (y, z): mul(halves[a][0], corners[0, y, z]) + mul(halves[a][1], corners[1, y, z])
            for y in range(2)
            for z in range(2)
        }
        for b in range(5):
            low, high = (
                mul(halves[b][0], plane[0, z]) + mul(halves[b][1], plane[1, z]) for z in range(2)
            )
            for c in range(5):
                visc[25 * a + 5 * b + c] = mul(halves[c][0], low) + mul(halves[c][1], high)


def span_flux_kernel(gs, eps, rcse, rcso, rse, rso, rce, rco, visc, fs, bso, bse):
    i, j = row_ids()
    is_low = j == 0
    es, ec = even_span(), even_chord()

    def sides(even, first, second):
        return (jnp.where(even, second, first), jnp.where(even, first, second))

    below, above = sides(ec, rce[CHORD_N], rco[CHORD_N])
    before, after = sides(es, rse[SPAN_N], rso[SPAN_N])
    low = [sides(es, rcse[n], rcso[n]) for n in range(2)]
    viscosity_into(
        visc, eps[...], below, above, before, after, (low[0][0], low[1][0]), (low[0][1], low[1][1])
    )
    weights = [jnp.where(is_low, float(0.5 * CORR_L[k]), float(0.5 * CORR_R[k])) for k in range(5)]

    def one(v, carry):
        received = {}

        def leaving(f):
            m, q = f // 2, f % 2
            if m not in received:
                base = v * SPAN_V + m
                received[m] = sides(es, rse[base], rso[base])
            edge = open_span(received[m][0], received[m][1], q, is_low)
            values = []
            for k, p in enumerate(line_points(1, f)):
                value = visc[p] * (gs[v, p] + weights[k] * edge)
                fs[v, p] = value
                values.append(value)
            left, right = traces(even_odd(values))
            return jnp.where(is_low, left, right)

        pack_span(leaving, is_low, es, bse, bso, v * SPAN_V)
        return carry

    lax.fori_loop(0, NV, one, 0)


def chord_flux_kernel(gc, visc, rce, rco, fc, bco, bce):
    i, _ = row_ids()
    first_row = i == 0
    ec = even_chord()
    weights = [
        jnp.where(i == 0, float(0.5 * CORR_L[k]), jnp.where(i == 3, float(0.5 * CORR_R[k]), 0.0))
        for k in range(5)
    ]

    def one(v, carry):
        received = {}

        def leaving(f):
            m, q = f // 4, f % 4
            if m not in received:
                base = v * CHORD_V + m
                first, second = rce[base], rco[base]
                received[m] = (jnp.where(ec, second, first), jnp.where(ec, first, second))
            edge = open_chord(received[m][0], received[m][1], q, i)
            values = []
            for k, p in enumerate(line_points(0, f)):
                value = visc[p] * (gc[v, p] + weights[k] * edge)
                fc[v, p] = value
                values.append(value)
            left, right = traces(even_odd(values))
            return jnp.where(first_row, left, right)

        pack_chord(leaving, i, ec, bce, bco, v * CHORD_V)
        return carry

    lax.fori_loop(0, NV, one, 0)


def divergence_kernel(gn, visc, fs, fc, res, total_ref, diff_ref):
    i, j = row_ids()
    lane = lane_ids()
    is_low = j == 0
    sign_row = jnp.where(is_low, 1.0, -1.0)

    def one(v, carry):
        def normal_flux(f):
            return even_odd([visc[p] * gn[v, p] for p in line_points(2, f)])

        for f in range(NF):
            left, right = traces(normal_flux(f))
            total_ref[f], diff_ref[f] = neighbours_normal(left, right, -1.0, lane)
        for axis, ref in ((0, fc), (1, fs), (2, gn)):
            for f in range(NF):
                points = line_points(axis, f)
                if axis == 2:
                    parts = normal_flux(f)
                    total, diff = total_ref[f], diff_ref[f]
                else:
                    parts = even_odd([ref[v, p] for p in points])
                    left, right = traces(parts)
                    if axis == 0:
                        total, diff = neighbours_chord(left, right, -1.0, i)
                    else:
                        total, diff = neighbours_span(left, right, is_low, sign_row)
                for p, value in zip(points, slope(parts, total, diff)):
                    res[v, p] = value if axis == 0 else res[v, p] + value
        return carry

    lax.fori_loop(0, NV, one, 0)


def close_kernel(res, rbse, rbso, rbce, rbco, out, span_edge, chord_edge):
    i, j = row_ids()
    is_low = j == 0
    es, ec = even_span(), even_chord()
    wspan = [jnp.where(is_low, float(0.5 * CORR_L[k]), float(0.5 * CORR_R[k])) for k in range(5)]
    wchord = [
        jnp.where(i == 0, float(0.5 * CORR_L[k]), jnp.where(i == 3, float(0.5 * CORR_R[k]), 0.0))
        for k in range(5)
    ]

    def one(v, carry):
        for f in range(NF):
            base = v * SPAN_V + f // 2
            first, second = rbse[base], rbso[base]
            span_edge[f] = open_span(
                jnp.where(es, second, first), jnp.where(es, first, second), f % 2, is_low
            )
            base = v * CHORD_V + f // 4
            first, second = rbce[base], rbco[base]
            chord_edge[f] = open_chord(
                jnp.where(ec, second, first), jnp.where(ec, first, second), f % 4, i
            )
        for a in range(5):
            for b in range(5):
                for c in range(5):
                    p = 25 * a + 5 * b + c
                    out[v, p] = res[v, p] + (
                        wspan[b] * span_edge[5 * a + c] + wchord[a] * chord_edge[5 * b + c]
                    )
        return carry

    lax.fori_loop(0, NV, one, 0)


def vec(*lead):
    return jax.ShapeDtypeStruct(lead + (ROWS, LANES), jnp.float32)


def call(kernel, name, outs, args, scratch=(), alias=None, cycles=1000):
    vmem = pl.BlockSpec(memory_space=pltpu.VMEM)
    total = sum(int(np.prod(x.shape)) for x in list(outs) + list(args)) * 4
    return pl.pallas_call(
        kernel,
        out_shape=outs,
        in_specs=[vmem] * len(args),
        out_specs=[vmem] * len(outs),
        scratch_shapes=[pltpu.VMEM(s.shape, s.dtype) for s in scratch],
        input_output_aliases=alias or {},
        compiler_params=pltpu.CompilerParams(vmem_limit_bytes=VMEM_LIMIT),
        cost_estimate=pl.CostEstimate(flops=cycles * 4096, bytes_accessed=total, transcendentals=0),
        name=name,
    )(*args)


VMEM_LIMIT = 24 * 2**20


def paired(n, odd, wraps):
    route = []
    for lower in range(odd, n, 2):
        upper = lower + 1
        if upper >= n:
            if not wraps:
                continue
            upper %= n
        route += [(lower, upper), (upper, lower)]
    return route


def shards(state):
    chords, spans = lax.axis_size("chord"), lax.axis_size("span")

    def span_swap(array, odd):
        return lax.ppermute(array, "span", paired(spans, odd, True))

    def chord_swap(array, odd):
        return lax.ppermute(array, "chord", paired(chords, odd, False))

    u = state.reshape(NV, 125, ROWS, LANES)
    so, se, co, ce, eps = call(
        leave_kernel,
        "leave",
        [vec(SPAN_N + 1), vec(SPAN_N + 1), vec(CHORD_N + 1), vec(CHORD_N + 1), vec()],
        [u],
        [vec(125)],
    )
    rso = span_swap(so, 1)
    rce = chord_swap(ce, 0)
    rco = chord_swap(co, 1)
    rse = span_swap(se, 0)
    gc, gs, gn = call(
        gradient_kernel, "gradient", [vec(NV, 125)] * 3, [u], [vec(NF), vec(NF)], cycles=5000
    )
    (cor,) = call(corner_kernel, "corner", [vec(2)], [rce, rco])
    rcse = span_swap(cor, 0)
    rcso = span_swap(cor, 1)
    visc, fs, bso, bse = call(
        span_flux_kernel,
        "span_flux",
        [vec(125), vec(NV, 125), vec(SPAN_N), vec(SPAN_N)],
        [gs, eps, rcse, rcso, rse, rso, rce, rco],
        alias={0: 1},
        cycles=2000,
    )
    rbso = span_swap(bso, 1)
    fc, bco, bce = call(
        chord_flux_kernel,
        "chord_flux",
        [vec(NV, 125), vec(CHORD_N), vec(CHORD_N)],
        [gc, visc, rce, rco],
        alias={0: 0},
        cycles=2000,
    )
    rbco = chord_swap(bco, 1)
    rbce = chord_swap(bce, 0)
    rbse = span_swap(bse, 0)
    (res,) = call(
        divergence_kernel,
        "divergence",
        [vec(NV, 125)],
        [gn, visc, fs, fc],
        [vec(NF), vec(NF)],
        cycles=6000,
    )
    (out,) = call(
        close_kernel,
        "close",
        [vec(NV, 125)],
        [res, rbse, rbso, rbce, rbco],
        [vec(NF), vec(NF)],
        alias={0: 0},
        cycles=2000,
    )
    return (out.reshape(state.shape), visc.reshape(state.shape[1:]))


def solution(mesh):
    in_specs = (P(None, None, "chord", "span", None),)
    out_specs = (P(None, None, "chord", "span", None), P(None, "chord", "span", None))
    return jax.shard_map(shards, mesh=mesh, in_specs=in_specs, out_specs=out_specs, check_vma=False)
```

```python
import math

import jax
import jax.numpy as jnp
import numpy as np
from jax import lax
from jax.experimental import pallas as pl
from jax.experimental.pallas import tpu as pltpu
from jax.sharding import PartitionSpec as P


EPS_SCALE = 0.01
SENSOR_CENTRE = -3.0
SENSOR_WIDTH = 1.5
RATIO_FLOOR = 1e-06
ENERGY_EPS = 1e-06
GAUSS_NODES = [-0.906179845938664, -0.5384693101056831, 0.0, 0.5384693101056831, 0.906179845938664]
GAUSS_WEIGHTS = [
    0.2369268850561891,
    0.4786286704993665,
    0.5688888888888889,
    0.4786286704993665,
    0.2369268850561891,
]


def legendre_values(points):
    values = [np.ones(points.shape), np.array(points)]
    for order in range(1, 5):
        values.append(
            ((2 * order + 1) * points * values[order] - order * values[order - 1]) / (order + 1)
        )
    return values


def line_tables():
    line_nodes = np.array(GAUSS_NODES)
    quadrature_weights = np.array(GAUSS_WEIGHTS)
    barycentric = np.array(
        [
            1.0 / np.prod([line_nodes[j] - line_nodes[k] for k in range(5) if k != j])
            for j in range(5)
        ]
    )
    derivative = np.zeros((5, 5))
    for i in range(5):
        for j in range(5):
            if i != j:
                derivative[i, j] = barycentric[j] / barycentric[i] / (line_nodes[i] - line_nodes[j])
        derivative[i, i] = -np.sum(derivative[i])
    left_values = np.ones(5)
    right_values = np.ones(5)
    for j in range(5):
        for k in range(5):
            if k != j:
                left_values[j] *= (-1.0 - line_nodes[k]) / (line_nodes[j] - line_nodes[k])
                right_values[j] *= (1.0 - line_nodes[k]) / (line_nodes[j] - line_nodes[k])
    legendre = legendre_values(line_nodes)
    fourth_slope = 7.0 * legendre[3] + 3.0 * legendre[1]
    fifth_slope = 9.0 * legendre[4] + 5.0 * legendre[2] + legendre[0]
    modal = np.zeros((5, 5))
    for k in range(5):
        modal[k, :] = quadrature_weights * math.sqrt((2 * k + 1) / 2.0) * legendre[k]
    return (line_nodes, derivative, left_values, right_values, fourth_slope, fifth_slope, modal)


NODES, DERIV, LEFT, RIGHT, SLOPE4, SLOPE5, MODAL = line_tables()
CORR_L = 0.5 * (SLOPE4 - SLOPE5)
CORR_R = 0.5 * (SLOPE4 + SLOPE5)
OWN = DERIV - 0.5 * (np.outer(CORR_L, LEFT) + np.outer(CORR_R, RIGHT))
ROWS, LANES = 8, 128
NV, NF = 5, 25
SPAN_V, CHORD_V = 13, 7
SPAN_N, CHORD_N = NV * SPAN_V, NV * CHORD_V


def mul(scale, x):
    return float(scale) * x


def even_odd(x):
    return (x[0] + x[4], x[1] + x[3], x[0] - x[4], x[1] - x[3], x[2])


def traces(parts):
    e0, e1, o0, o1, c = parts
    even = (
        mul(0.5 * (LEFT[0] + LEFT[4]), e0) + mul(0.5 * (LEFT[1] + LEFT[3]), e1) + mul(LEFT[2], c)
    )
    odd = mul(0.5 * (LEFT[0] - LEFT[4]), o0) + mul(0.5 * (LEFT[1] - LEFT[3]), o1)
    return (even + odd, even - odd)


def slope(parts, total, diff):
    e0, e1, o0, o1, c = parts
    even, odd = [], []
    for i in range(3):
        even.append(
            mul(0.5 * (OWN[i, 0] - OWN[i, 4]), o0)
            + mul(0.5 * (OWN[i, 1] - OWN[i, 3]), o1)
            + mul(0.25 * SLOPE5[i], diff)
        )
    for i in range(2):
        odd.append(
            mul(0.5 * (OWN[i, 0] + OWN[i, 4]), e0)
            + mul(0.5 * (OWN[i, 1] + OWN[i, 3]), e1)
            + (mul(OWN[i, 2], c) + mul(0.25 * SLOPE4[i], total))
        )
    return [
        even[0] + odd[0],
        even[1] + odd[1],
        even[2],
        even[1] - odd[1],
        even[0] - odd[0],
    ]


def modal_line(x):
    e0, e1, o0, o1, c = even_odd(x)
    out = []
    for k in range(5):
        if k % 2 == 0:
            out.append(mul(MODAL[k, 0], e0) + mul(MODAL[k, 1], e1) + mul(MODAL[k, 2], c))
        else:
            out.append(mul(MODAL[k, 0], o0) + mul(MODAL[k, 1], o1))
    return out


def line_points(axis, f):
    a, b = f // 5, f % 5
    if axis == 0:
        return [25 * k + 5 * a + b for k in range(5)]
    if axis == 1:
        return [25 * a + 5 * k + b for k in range(5)]
    return [25 * a + 5 * b + k for k in range(5)]


def row_ids():
    rows = lax.broadcasted_iota(jnp.int32, (ROWS, LANES), 0)
    return (rows // 2, rows % 2)


def lane_ids():
    return lax.broadcasted_iota(jnp.int32, (ROWS, LANES), 1)


def up_rows(x, n):
    n = n % ROWS
    return x if n == 0 else pltpu.roll(x, n, 0)


def splat_flag(flag):
    return jnp.full((ROWS, LANES), flag.astype(jnp.int32), jnp.int32) > 0


def chord_ends():
    at = lax.axis_index("chord")
    return (splat_flag(at == 0), splat_flag(at == lax.axis_size("chord") - 1))


def even_span():
    return splat_flag(lax.axis_index("span") % 2 == 0)


def even_chord():
    return splat_flag(lax.axis_index("chord") % 2 == 0)


def pack_span(out_of, is_low, even, first_ref, second_ref, base):
    for m in range(SPAN_V):
        f0 = out_of(2 * m)
        f1 = out_of(2 * m + 1) if 2 * m + 1 < NF else f0
        up = jnp.where(is_low, up_rows(f0, -1), f1)
        down = jnp.where(is_low, f0, up_rows(f1, 1))
        first_ref[base + m] = jnp.where(even, up, down)
        second_ref[base + m] = jnp.where(even, down, up)


def pack_chord(out_of, i, even, first_ref, second_ref, base):
    for m in range(CHORD_V):
        up = down = None
        for q in range(4):
            f = 4 * m + q
            if f >= NF:
                continue
            trace = out_of(f)
            u, d = up_rows(trace, 2 * q - 6), up_rows(trace, 2 * q)
            up = u if up is None else jnp.where(i == q, u, up)
            down = d if down is None else jnp.where(i == q, d, down)
        first_ref[base + m] = jnp.where(even, up, down)
        second_ref[base + m] = jnp.where(even, down, up)


def open_span(below, above, q, is_low):
    if q == 0:
        return jnp.where(is_low, below, up_rows(above, 1))
    return jnp.where(is_low, up_rows(below, -1), above)


def open_chord(below, above, q, i):
    return jnp.where(i == 0, up_rows(below, -2 * q), up_rows(above, 6 - 2 * q))


def sided(even, first, second):
    return (jnp.where(even, second, first), jnp.where(even, first, second))


def leave_span_kernel(source, so, se, eps_ref, state, work, sems):
    reads = [pltpu.make_async_copy(source.at[v], state.at[v], sems.at[v]) for v in range(NV)]
    for read in reads:
        read.start()
    _, j = row_ids()
    is_low = j == 0
    es = even_span()

    def one(v, carry):
        def leaving(f):
            left, right = traces(even_odd([state[v, p] for p in line_points(1, f)]))
            return jnp.where(is_low, left, right)

        pack_span(leaving, is_low, es, se, so, v * SPAN_V)
        return carry

    reads[0].wait()
    eps = sensor(state, work)
    eps_ref[...] = eps
    se[SPAN_N] = eps
    one(0, 0)

    def later(v, carry):
        pltpu.make_async_copy(source.at[v], state.at[v], sems.at[v]).wait()
        return one(v, carry)

    lax.fori_loop(1, NV, later, 0)


def leave_chord_kernel(state, eps, rkso, rse, co, ce):
    i, _ = row_ids()
    first_row = i == 0
    ec = even_chord()

    def one(v, carry):
        def leaving(f):
            left, right = traces(even_odd([state[v, p] for p in line_points(0, f)]))
            return jnp.where(first_row, left, right)

        pack_chord(leaving, i, ec, ce, co, v * CHORD_V)
        return carry

    lax.fori_loop(0, NV, one, 0)
    before, after = sided(even_span(), rse[SPAN_N], rkso[...])
    for ref in (co, ce):
        ref[CHORD_N], ref[CHORD_N + 1], ref[CHORD_N + 2] = eps[...], before, after


def sensor(state, work):
    for axis in range(2):
        origin = state.at[0] if axis == 0 else work
        for f in range(NF):
            points = line_points(axis, f)
            for p, value in zip(points, modal_line([origin[p] for p in points])):
                work[p] = value
    low_sums, high_sums = [], []
    for f in range(NF):
        a, b = f // 5, f % 5
        low, high = None, None
        for k, value in enumerate(modal_line([work[p] for p in line_points(2, f)])):
            square = value * value
            if a == 4 or b == 4 or k == 4:
                high = square if high is None else high + square
            else:
                low = square if low is None else low + square
        if low is not None:
            low_sums.append(low)
        high_sums.append(high)

    def tree(values):
        while len(values) > 1:
            values = [
                values[n] + values[n + 1] if n + 1 < len(values) else values[n]
                for n in range(0, len(values), 2)
            ]
        return values[0]

    high_part = tree(high_sums)
    total = (tree(low_sums) + high_part) + ENERGY_EPS
    level = jnp.log(jnp.maximum(high_part / total, RATIO_FLOOR)) * (1.0 / math.log(10.0))
    ramp = jnp.clip((level - SENSOR_CENTRE) / SENSOR_WIDTH, -1.0, 1.0)
    eps = EPS_SCALE * 0.5 * (1.0 + jnp.sin(0.5 * math.pi * ramp))
    return eps


def neighbours_chord(left, right, sign, i):
    first = (lax.axis_index("chord") == 0).astype(jnp.float32) * sign
    last = (lax.axis_index("chord") == lax.axis_size("chord") - 1).astype(jnp.float32) * sign
    before = jnp.where(i == 0, left * first, up_rows(right, 2))
    after = jnp.where(i == 3, right * last, up_rows(left, -2))
    return (before + after, after - before)


def neighbours_span(left, right, is_low, sign_row):
    inner = jnp.where(is_low, up_rows(left, -1), up_rows(right, 1))
    return (inner, inner * sign_row)


def neighbours_normal(left, right, sign, lane):
    before = jnp.where(lane == 0, mul(sign, left), pltpu.roll(right, 1, 1))
    after = jnp.where(lane == LANES - 1, mul(sign, right), pltpu.roll(left, LANES - 1, 1))
    return (before + after, after - before)


def gradient_kernel(state, gc, gs, gn, total_ref, diff_ref):
    i, j = row_ids()
    lane = lane_ids()
    is_low = j == 0
    sign_row = jnp.where(is_low, 1.0, -1.0)

    def one(v, carry):
        def lines(axis, f):
            return even_odd([state[v, p] for p in line_points(axis, f)])

        for f in range(NF):
            left, right = traces(lines(2, f))
            total_ref[f], diff_ref[f] = neighbours_normal(left, right, 1.0, lane)
        for axis, ref in ((0, gc), (1, gs), (2, gn)):
            for f in range(NF):
                parts = lines(axis, f)
                if axis == 2:
                    total, diff = total_ref[f], diff_ref[f]
                else:
                    left, right = traces(parts)
                    if axis == 0:
                        total, diff = neighbours_chord(left, right, 1.0, i)
                    else:
                        total, diff = neighbours_span(left, right, is_low, sign_row)
                for p, value in zip(line_points(axis, f), slope(parts, total, diff)):
                    ref[v, p] = value
        return carry

    lax.fori_loop(0, NV, one, 0)


def viscosity_into(visc, own, behind, ahead):
    i, j = row_ids()
    lane = lane_ids()
    is_low = j == 0

    def chord_pair(mid, low, high):
        under = up_rows(jnp.where(i == 3, low, mid), 2)
        over = up_rows(jnp.where(i == 0, high, mid), -2)
        return (jnp.maximum(mid, under), jnp.maximum(mid, over))

    mids, befores, afters = (chord_pair(own[n], behind[n], ahead[n]) for n in range(3))
    corners = {}
    for x in range(2):
        mid, low, high = mids[x], befores[x], afters[x]
        under = jnp.where(is_low, up_rows(low, -1), up_rows(mid, 1))
        over = jnp.where(is_low, up_rows(mid, -1), up_rows(high, 1))
        for y, value in enumerate((jnp.maximum(mid, under), jnp.maximum(mid, over))):
            low_z = jnp.where(lane == 0, value, pltpu.roll(value, 1, 1))
            high_z = jnp.where(lane == LANES - 1, value, pltpu.roll(value, LANES - 1, 1))
            corners[x, y, 0] = jnp.maximum(value, low_z)
            corners[x, y, 1] = jnp.maximum(value, high_z)
    halves = [((1.0 - x) / 2.0, (1.0 + x) / 2.0) for x in NODES]
    for a in range(5):
        plane = {
            (y, z): mul(halves[a][0], corners[0, y, z]) + mul(halves[a][1], corners[1, y, z])
            for y in range(2)
            for z in range(2)
        }
        for b in range(5):
            low, high = (
                mul(halves[b][0], plane[0, z]) + mul(halves[b][1], plane[1, z]) for z in range(2)
            )
            for c in range(5):
                visc[25 * a + 5 * b + c] = mul(halves[c][0], low) + mul(halves[c][1], high)


def span_flux_kernel(gs, visc, rse, rso, fs, bso, bse):
    _, j = row_ids()
    is_low = j == 0
    es, ec = even_span(), even_chord()

    weights = span_weights(is_low)

    def one(v, carry):
        received = {}

        def leaving(f):
            m, q = f // 2, f % 2
            if m not in received:
                base = v * SPAN_V + m
                received[m] = sided(es, rse[base], rso[base])
            edge = open_span(received[m][0], received[m][1], q, is_low)
            values = []
            for k, p in enumerate(line_points(1, f)):
                value = visc[p] * (gs[v, p] + weights[k] * edge)
                fs[v, p] = value
                values.append(value)
            left, right = traces(even_odd(values))
            return jnp.where(is_low, left, right)

        pack_span(leaving, is_low, es, bse, bso, v * SPAN_V)
        return carry

    lax.fori_loop(0, NV, one, 0)


def chord_flux_kernel(gc, eps, rkso, rse, rce, rco, visc, fc, bco, bce):
    i, _ = row_ids()
    first_row = i == 0
    es, ec = even_span(), even_chord()
    before, after = sided(es, rse[SPAN_N], rkso[...])
    first, last = chord_ends()
    low, high = [], []
    for n in range(3):
        behind, ahead = sided(ec, rce[CHORD_N + n], rco[CHORD_N + n])
        low.append(jnp.where(first, 0.0, behind))
        high.append(jnp.where(last, 0.0, ahead))
    viscosity_into(visc, (eps[...], before, after), low, high)
    weights = chord_weights(i)

    def one(v, carry):
        received = {}

        def leaving(f):
            m, q = f // 4, f % 4
            if m not in received:
                base = v * CHORD_V + m
                first, second = rce[base], rco[base]
                received[m] = (jnp.where(ec, second, first), jnp.where(ec, first, second))
            edge = open_chord(received[m][0], received[m][1], q, i)
            values = []
            for k, p in enumerate(line_points(0, f)):
                value = visc[p] * (gc[v, p] + weights[k] * edge)
                fc[v, p] = value
                values.append(value)
            left, right = traces(even_odd(values))
            return jnp.where(first_row, left, right)

        pack_chord(leaving, i, ec, bce, bco, v * CHORD_V)
        return carry

    lax.fori_loop(0, NV, one, 0)


def divergence_kernel(gn, visc, fs, fc, res, visc_out, total_ref, diff_ref, sem):
    write = pltpu.make_async_copy(visc, visc_out, sem)
    write.start()
    i, j = row_ids()
    lane = lane_ids()
    is_low = j == 0
    sign_row = jnp.where(is_low, 1.0, -1.0)

    def one(v, carry):
        def normal_flux(f):
            return even_odd([visc[p] * gn[v, p] for p in line_points(2, f)])

        for f in range(NF):
            left, right = traces(normal_flux(f))
            total_ref[f], diff_ref[f] = neighbours_normal(left, right, -1.0, lane)
        for axis, ref in ((0, fc), (1, fs), (2, gn)):
            for f in range(NF):
                points = line_points(axis, f)
                if axis == 2:
                    parts = normal_flux(f)
                    total, diff = total_ref[f], diff_ref[f]
                else:
                    parts = even_odd([ref[v, p] for p in points])
                    left, right = traces(parts)
                    if axis == 0:
                        total, diff = neighbours_chord(left, right, -1.0, i)
                    else:
                        total, diff = neighbours_span(left, right, is_low, sign_row)
                for p, value in zip(points, slope(parts, total, diff)):
                    res[v, p] = value if axis == 0 else res[v, p] + value
        return carry

    lax.fori_loop(0, NV, one, 0)
    write.wait()


def close_chord_kernel(res, rbce, rbco, out, edge):
    i, _ = row_ids()
    ec = even_chord()
    weights = chord_weights(i)

    def one(v, carry):
        for m in range(CHORD_V):
            first, second = rbce[v * CHORD_V + m], rbco[v * CHORD_V + m]
            behind, ahead = jnp.where(ec, second, first), jnp.where(ec, first, second)
            for f in range(4 * m, min(4 * m + 4, NF)):
                edge[f] = open_chord(behind, ahead, f % 4, i)
        for f in range(NF):
            for k, p in enumerate(line_points(0, f)):
                out[v, p] = res[v, p] + weights[k] * edge[f]
        return carry

    lax.fori_loop(0, NV, one, 0)


def close_span_kernel(res, rbse, rbso, final, edge, out, sems):
    _, j = row_ids()
    is_low = j == 0
    es = even_span()
    weights = span_weights(is_low)

    def send(v):
        return pltpu.make_async_copy(out.at[v], final.at[v], sems.at[v])

    def one(v, carry):
        for m in range(SPAN_V):
            first, second = rbse[v * SPAN_V + m], rbso[v * SPAN_V + m]
            behind, ahead = jnp.where(es, second, first), jnp.where(es, first, second)
            for f in range(2 * m, min(2 * m + 2, NF)):
                edge[f] = open_span(behind, ahead, f % 2, is_low)
        for f in range(NF):
            for k, p in enumerate(line_points(1, f)):
                out[v, p] = res[v, p] + weights[k] * edge[f]

        @pl.when(v > 0)
        def _():
            send(v - 1).start()

        return carry

    lax.fori_loop(0, NV, one, 0)
    send(NV - 1).start()
    for v in range(NV):
        send(v).wait()


def span_weights(is_low):
    return [jnp.where(is_low, float(0.5 * CORR_L[k]), float(0.5 * CORR_R[k])) for k in range(5)]


def chord_weights(i):
    first, last = chord_ends()
    low, high = jnp.logical_and(i == 0, ~first), jnp.logical_and(i == 3, ~last)
    return [
        jnp.where(low, float(0.5 * CORR_L[k]), jnp.where(high, float(0.5 * CORR_R[k]), 0.0))
        for k in range(5)
    ]


def held(*lead):
    return pltpu.VMEM(lead + (ROWS, LANES), jnp.float32)


def vec(*lead):
    return jax.ShapeDtypeStruct(lead + (ROWS, LANES), jnp.float32)


def call(kernel, outs, args, scratch=(), cycles=1000, far_in=(), far_out=(), grant=24 * 2**20):
    vmem, hbm = (pl.BlockSpec(memory_space=m) for m in (pltpu.VMEM, pltpu.HBM))
    total = sum(int(np.prod(x.shape)) for x in list(outs) + list(args)) * 4
    return pl.pallas_call(
        kernel,
        out_shape=outs,
        in_specs=[hbm if n in far_in else vmem for n in range(len(args))],
        out_specs=[hbm if n in far_out else vmem for n in range(len(outs))],
        scratch_shapes=list(scratch),
        compiler_params=pltpu.CompilerParams(vmem_limit_bytes=grant),
        cost_estimate=pl.CostEstimate(flops=cycles * 4096, bytes_accessed=total, transcendentals=0),
    )(*args)


def paired(n, odd, wraps):
    route = []
    for lower in range(odd, n, 2):
        upper = lower + 1
        if upper >= n:
            if not wraps:
                continue
            upper %= n
        route += [(lower, upper), (upper, lower)]
    return route


def shards(state):
    chords, spans = lax.axis_size("chord"), lax.axis_size("span")

    def span_swap(array, odd):
        return lax.ppermute(array, "span", paired(spans, odd, True))

    def chord_swap(array, odd):
        route = [
            (a * spans + c, b * spans + c) for a, b in paired(chords, odd, False) for c in range(spans)
        ]
        if odd:
            route += [
                (a * spans + c, a * spans + (c ^ 1)) for a in (0, chords - 1) for c in range(spans)
            ]
        return lax.ppermute(array, ("chord", "span"), route)

    dma = pltpu.SemaphoreType.DMA
    u = state.reshape(NV, 125, ROWS, LANES)
    so, se, eps, near = call(
        leave_span_kernel,
        [vec(SPAN_N), vec(SPAN_N + 1), vec(), vec(NV, 125)],
        [pltpu.with_memory_space_constraint(u, pltpu.HBM)],
        [held(125), dma((NV,))],
        far_in=(0,),
    )
    rkso = span_swap(eps, 1)
    rse = span_swap(se, 0)
    rso = span_swap(so, 1)
    co, ce = call(leave_chord_kernel, [vec(CHORD_N + 3), vec(CHORD_N + 3)], [near, eps, rkso, rse])
    rco = chord_swap(co, 1)
    rce = chord_swap(ce, 0)
    gc, gs, gn = call(
        gradient_kernel, [vec(NV, 125)] * 3, [near], [held(NF), held(NF)], cycles=5000
    )
    visc, fc, bco, bce = call(
        chord_flux_kernel,
        [vec(125), vec(NV, 125), vec(CHORD_N), vec(CHORD_N)],
        [gc, eps, rkso, rse, rce, rco],
        cycles=2000,
    )
    rbco = chord_swap(bco, 1)
    fs, bso, bse = call(
        span_flux_kernel,
        [vec(NV, 125), vec(SPAN_N), vec(SPAN_N)],
        [gs, visc, rse, rso],
        cycles=2000,
    )
    rbso = span_swap(bso, 1)
    rbse = span_swap(bse, 0)
    rbce = chord_swap(bce, 0)
    res, visc_out = call(
        divergence_kernel,
        [vec(NV, 125), vec(125)],
        [gn, visc, fs, fc],
        [held(NF), held(NF), dma(())],
        cycles=6000,
        far_out=(1,),
    )
    (res,) = call(close_chord_kernel, [vec(NV, 125)], [res, rbce, rbco], [held(NF)], cycles=1000)
    (out,) = call(
        close_span_kernel,
        [vec(NV, 125)],
        [res, rbse, rbso],
        [held(NF), held(NV, 125), dma((NV,))],
        cycles=2000,
        far_out=(0,),
    )
    return (out.reshape(state.shape), visc_out.reshape(state.shape[1:]))


def solution(mesh):
    in_specs = (P(None, None, "chord", "span", None),)
    out_specs = (P(None, None, "chord", "span", None), P(None, "chord", "span", None))

    return jax.shard_map(shards, mesh=mesh, in_specs=in_specs, out_specs=out_specs, check_vma=False)
```

```python
import math

import jax
import jax.numpy as jnp
import numpy as np
from jax import lax
from jax.experimental import pallas as pl
from jax.experimental.pallas import tpu as pltpu
from jax.sharding import PartitionSpec as P


EPS_SCALE = 0.01
SENSOR_CENTRE = -3.0
SENSOR_WIDTH = 1.5
RATIO_FLOOR = 1e-06
ENERGY_EPS = 1e-06
GAUSS_NODES = [-0.906179845938664, -0.5384693101056831, 0.0, 0.5384693101056831, 0.906179845938664]
GAUSS_WEIGHTS = [
    0.2369268850561891,
    0.4786286704993665,
    0.5688888888888889,
    0.4786286704993665,
    0.2369268850561891,
]


def legendre_values(points):
    values = [np.ones(points.shape), np.array(points)]
    for order in range(1, 5):
        values.append(
            ((2 * order + 1) * points * values[order] - order * values[order - 1]) / (order + 1)
        )
    return values


def line_tables():
    line_nodes = np.array(GAUSS_NODES)
    quadrature_weights = np.array(GAUSS_WEIGHTS)
    barycentric = np.array(
        [
            1.0 / np.prod([line_nodes[j] - line_nodes[k] for k in range(5) if k != j])
            for j in range(5)
        ]
    )
    derivative = np.zeros((5, 5))
    for i in range(5):
        for j in range(5):
            if i != j:
                derivative[i, j] = barycentric[j] / barycentric[i] / (line_nodes[i] - line_nodes[j])
        derivative[i, i] = -np.sum(derivative[i])
    left_values = np.ones(5)
    right_values = np.ones(5)
    for j in range(5):
        for k in range(5):
            if k != j:
                left_values[j] *= (-1.0 - line_nodes[k]) / (line_nodes[j] - line_nodes[k])
                right_values[j] *= (1.0 - line_nodes[k]) / (line_nodes[j] - line_nodes[k])
    legendre = legendre_values(line_nodes)
    fourth_slope = 7.0 * legendre[3] + 3.0 * legendre[1]
    fifth_slope = 9.0 * legendre[4] + 5.0 * legendre[2] + legendre[0]
    modal = np.zeros((5, 5))
    for k in range(5):
        modal[k, :] = quadrature_weights * math.sqrt((2 * k + 1) / 2.0) * legendre[k]
    return (line_nodes, derivative, left_values, right_values, fourth_slope, fifth_slope, modal)


NODES, DERIV, LEFT, RIGHT, SLOPE4, SLOPE5, MODAL = line_tables()
CORR_L = 0.5 * (SLOPE4 - SLOPE5)
CORR_R = 0.5 * (SLOPE4 + SLOPE5)
OWN = DERIV - 0.5 * (np.outer(CORR_L, LEFT) + np.outer(CORR_R, RIGHT))
ROWS, LANES = 8, 128
NV, NF = 5, 25
SPAN_V, CHORD_V = 13, 7
SPAN_N, CHORD_N = NV * SPAN_V, NV * CHORD_V


def mul(scale, x):
    return float(scale) * x


def even_odd(x):
    return (x[0] + x[4], x[1] + x[3], x[0] - x[4], x[1] - x[3], x[2])


def traces(parts):
    e0, e1, o0, o1, c = parts
    even = (
        mul(0.5 * (LEFT[0] + LEFT[4]), e0) + mul(0.5 * (LEFT[1] + LEFT[3]), e1) + mul(LEFT[2], c)
    )
    odd = mul(0.5 * (LEFT[0] - LEFT[4]), o0) + mul(0.5 * (LEFT[1] - LEFT[3]), o1)
    return (even + odd, even - odd)


def slope(parts, total, diff):
    e0, e1, o0, o1, c = parts
    even, odd = [], []
    for i in range(3):
        even.append(
            mul(0.5 * (OWN[i, 0] - OWN[i, 4]), o0)
            + mul(0.5 * (OWN[i, 1] - OWN[i, 3]), o1)
            + mul(0.25 * SLOPE5[i], diff)
        )
    for i in range(2):
        odd.append(
            mul(0.5 * (OWN[i, 0] + OWN[i, 4]), e0)
            + mul(0.5 * (OWN[i, 1] + OWN[i, 3]), e1)
            + (mul(OWN[i, 2], c) + mul(0.25 * SLOPE4[i], total))
        )
    return [
        even[0] + odd[0],
        even[1] + odd[1],
        even[2],
        even[1] - odd[1],
        even[0] - odd[0],
    ]


def modal_line(x):
    e0, e1, o0, o1, c = even_odd(x)
    out = []
    for k in range(5):
        if k % 2 == 0:
            out.append(mul(MODAL[k, 0], e0) + mul(MODAL[k, 1], e1) + mul(MODAL[k, 2], c))
        else:
            out.append(mul(MODAL[k, 0], o0) + mul(MODAL[k, 1], o1))
    return out


def line_points(axis, f):
    a, b = f // 5, f % 5
    if axis == 0:
        return [25 * k + 5 * a + b for k in range(5)]
    if axis == 1:
        return [25 * a + 5 * k + b for k in range(5)]
    return [25 * a + 5 * b + k for k in range(5)]


def row_ids():
    rows = lax.broadcasted_iota(jnp.int32, (ROWS, LANES), 0)
    return (rows // 2, rows % 2)


def lane_ids():
    return lax.broadcasted_iota(jnp.int32, (ROWS, LANES), 1)


def up_rows(x, n):
    n = n % ROWS
    return x if n == 0 else pltpu.roll(x, n, 0)


def splat_flag(flag):
    return jnp.full((ROWS, LANES), flag.astype(jnp.int32), jnp.int32) > 0


def chord_ends():
    at = lax.axis_index("chord")
    return (splat_flag(at == 0), splat_flag(at == lax.axis_size("chord") - 1))


def even_span():
    return splat_flag(lax.axis_index("span") % 2 == 0)


def even_chord():
    return splat_flag(lax.axis_index("chord") % 2 == 0)


def pack_span(out_of, is_low, even, first_ref, second_ref, base):
    for m in range(SPAN_V):
        f0 = out_of(2 * m)
        f1 = out_of(2 * m + 1) if 2 * m + 1 < NF else f0
        up = jnp.where(is_low, up_rows(f0, -1), f1)
        down = jnp.where(is_low, f0, up_rows(f1, 1))
        first_ref[base + m] = jnp.where(even, up, down)
        second_ref[base + m] = jnp.where(even, down, up)


def pack_chord(out_of, i, even, first_ref, second_ref, base):
    for m in range(CHORD_V):
        up = down = None
        for q in range(4):
            f = 4 * m + q
            if f >= NF:
                continue
            trace = out_of(f)
            u, d = up_rows(trace, 2 * q - 6), up_rows(trace, 2 * q)
            up = u if up is None else jnp.where(i == q, u, up)
            down = d if down is None else jnp.where(i == q, d, down)
        first_ref[base + m] = jnp.where(even, up, down)
        second_ref[base + m] = jnp.where(even, down, up)


def open_span(below, above, q, is_low):
    if q == 0:
        return jnp.where(is_low, below, up_rows(above, 1))
    return jnp.where(is_low, up_rows(below, -1), above)


def open_chord(below, above, q, i):
    return jnp.where(i == 0, up_rows(below, -2 * q), up_rows(above, 6 - 2 * q))


def sided(even, first, second):
    return (jnp.where(even, second, first), jnp.where(even, first, second))


def sensor_kernel(source, eps, density, work, sem):
    read = pltpu.make_async_copy(source.at[0], density, sem)
    read.start()
    read.wait()
    eps[...] = sensor(density, work)


def leave_span_kernel(state, so, se):
    _, j = row_ids()
    is_low = j == 0
    es = even_span()

    def one(v, carry):
        def leaving(f):
            left, right = traces(even_odd([state[v, p] for p in line_points(1, f)]))
            return jnp.where(is_low, left, right)

        pack_span(leaving, is_low, es, se, so, v * SPAN_V)
        return carry

    lax.fori_loop(0, NV, one, 0)


def leave_chord_kernel(state, eps, rkce, rkco, se, co, ce, se_three, three):
    i, _ = row_ids()
    first_row = i == 0
    ec = even_chord()

    def one(v, carry):
        def leaving(f):
            left, right = traces(even_odd([state[v, p] for p in line_points(0, f)]))
            return jnp.where(first_row, left, right)

        pack_chord(leaving, i, ec, ce, co, v * CHORD_V)
        return carry

    lax.fori_loop(0, NV, one, 0)
    first, last = chord_ends()
    behind, ahead = sided(ec, rkce[...], rkco[...])
    values = (eps[...], jnp.where(first, 0.0, behind), jnp.where(last, 0.0, ahead))
    for n, value in enumerate(values):
        three[n] = value
        se_three[SPAN_N + n] = value
    for m in range(SPAN_N):
        se_three[m] = se[m]


def sensor(density, work):
    for axis in range(2):
        origin = density if axis == 0 else work
        for f in range(NF):
            points = line_points(axis, f)
            for p, value in zip(points, modal_line([origin[p] for p in points])):
                work[p] = value
    low_sums, high_sums = [], []
    for f in range(NF):
        a, b = f // 5, f % 5
        low, high = None, None
        for k, value in enumerate(modal_line([work[p] for p in line_points(2, f)])):
            square = value * value
            if a == 4 or b == 4 or k == 4:
                high = square if high is None else high + square
            else:
                low = square if low is None else low + square
        if low is not None:
            low_sums.append(low)
        high_sums.append(high)

    def tree(values):
        while len(values) > 1:
            values = [
                values[n] + values[n + 1] if n + 1 < len(values) else values[n]
                for n in range(0, len(values), 2)
            ]
        return values[0]

    high_part = tree(high_sums)
    total = (tree(low_sums) + high_part) + ENERGY_EPS
    level = jnp.log(jnp.maximum(high_part / total, RATIO_FLOOR)) * (1.0 / math.log(10.0))
    ramp = jnp.clip((level - SENSOR_CENTRE) / SENSOR_WIDTH, -1.0, 1.0)
    eps = EPS_SCALE * 0.5 * (1.0 + jnp.sin(0.5 * math.pi * ramp))
    return eps


def neighbours_chord(left, right, sign, i):
    first = (lax.axis_index("chord") == 0).astype(jnp.float32) * sign
    last = (lax.axis_index("chord") == lax.axis_size("chord") - 1).astype(jnp.float32) * sign
    before = jnp.where(i == 0, left * first, up_rows(right, 2))
    after = jnp.where(i == 3, right * last, up_rows(left, -2))
    return (before + after, after - before)


def neighbours_span(left, right, is_low, sign_row):
    inner = jnp.where(is_low, up_rows(left, -1), up_rows(right, 1))
    return (inner, inner * sign_row)


def neighbours_normal(left, right, sign, lane):
    before = jnp.where(lane == 0, mul(sign, left), pltpu.roll(right, 1, 1))
    after = jnp.where(lane == LANES - 1, mul(sign, right), pltpu.roll(left, LANES - 1, 1))
    return (before + after, after - before)


def gradient_kernel(state, gc, gs):
    i, j = row_ids()
    is_low = j == 0
    sign_row = jnp.where(is_low, 1.0, -1.0)

    def one(v, carry):
        for axis, ref in ((0, gc), (1, gs)):
            for f in range(NF):
                points = line_points(axis, f)
                parts = even_odd([state[v, p] for p in points])
                left, right = traces(parts)
                if axis == 0:
                    total, diff = neighbours_chord(left, right, 1.0, i)
                else:
                    total, diff = neighbours_span(left, right, is_low, sign_row)
                for p, value in zip(points, slope(parts, total, diff)):
                    ref[v, p] = value
        return carry

    lax.fori_loop(0, NV, one, 0)


def viscosity_into(visc, own, behind, ahead):
    i, j = row_ids()
    lane = lane_ids()
    is_low = j == 0

    def chord_pair(mid, low, high):
        under = up_rows(jnp.where(i == 3, low, mid), 2)
        over = up_rows(jnp.where(i == 0, high, mid), -2)
        return (jnp.maximum(mid, under), jnp.maximum(mid, over))

    mids, befores, afters = (chord_pair(own[n], behind[n], ahead[n]) for n in range(3))
    corners = {}
    for x in range(2):
        mid, low, high = mids[x], befores[x], afters[x]
        under = jnp.where(is_low, up_rows(low, -1), up_rows(mid, 1))
        over = jnp.where(is_low, up_rows(mid, -1), up_rows(high, 1))
        for y, value in enumerate((jnp.maximum(mid, under), jnp.maximum(mid, over))):
            low_z = jnp.where(lane == 0, value, pltpu.roll(value, 1, 1))
            high_z = jnp.where(lane == LANES - 1, value, pltpu.roll(value, LANES - 1, 1))
            corners[x, y, 0] = jnp.maximum(value, low_z)
            corners[x, y, 1] = jnp.maximum(value, high_z)
    halves = [((1.0 - x) / 2.0, (1.0 + x) / 2.0) for x in NODES]
    for a in range(5):
        plane = {
            (y, z): mul(halves[a][0], corners[0, y, z]) + mul(halves[a][1], corners[1, y, z])
            for y in range(2)
            for z in range(2)
        }
        for b in range(5):
            low, high = (
                mul(halves[b][0], plane[0, z]) + mul(halves[b][1], plane[1, z]) for z in range(2)
            )
            for c in range(5):
                visc[25 * a + 5 * b + c] = mul(halves[c][0], low) + mul(halves[c][1], high)


def chord_send_kernel(gc, three, rkso, rse, visc, bco, bce):
    i, _ = row_ids()
    first_row = i == 0
    es, ec = even_span(), even_chord()
    viscosity_into(
        visc, *((three[n],) + sided(es, rse[SPAN_N + n], rkso[n]) for n in range(3))
    )

    def one(v, carry):
        def leaving(f):
            left, right = traces(even_odd([visc[p] * gc[v, p] for p in line_points(0, f)]))
            return jnp.where(first_row, left, right)

        pack_chord(leaving, i, ec, bce, bco, v * CHORD_V)
        return carry

    lax.fori_loop(0, NV, one, 0)
    share = 0.5 * LEFT * CORR_L

    def factor(f):
        e0, e1, o0, o1, c = even_odd([visc[p] for p in line_points(0, f)])
        even = (
            mul(0.5 * (share[0] + share[4]), e0)
            + mul(0.5 * (share[1] + share[3]), e1)
            + mul(share[2], c)
        )
        odd = mul(0.5 * (share[0] - share[4]), o0) + mul(0.5 * (share[1] - share[3]), o1)
        return jnp.where(first_row, odd + even, odd - even)

    pack_chord(factor, i, ec, bce, bco, CHORD_N)


def span_flux_kernel(gs, visc, rse, rso, fs, bso, bse):
    _, j = row_ids()
    is_low = j == 0
    es = even_span()
    weights = span_weights(is_low)

    def one(v, carry):
        received = {}

        def leaving(f):
            m, q = f // 2, f % 2
            if m not in received:
                base = v * SPAN_V + m
                received[m] = sided(es, rse[base], rso[base])
            edge = open_span(received[m][0], received[m][1], q, is_low)
            values = []
            for k, p in enumerate(line_points(1, f)):
                value = visc[p] * (gs[v, p] + weights[k] * edge)
                fs[v, p] = value
                values.append(value)
            left, right = traces(even_odd(values))
            return jnp.where(is_low, left, right)

        pack_span(leaving, is_low, es, bse, bso, v * SPAN_V)
        return carry

    lax.fori_loop(0, NV, one, 0)


def inner_kernel(state, visc, fs, gc, rce, rco, res, visc_out, total_ref, diff_ref, flux, sem):
    write = pltpu.make_async_copy(visc, visc_out, sem)
    write.start()
    i, j = row_ids()
    lane = lane_ids()
    is_low = j == 0
    sign_row = jnp.where(is_low, 1.0, -1.0)
    ec = even_chord()
    weights = chord_weights(i)

    def one(v, carry):
        received = {}

        def across(c):
            plane = {}
            for b in range(5):
                f = 5 * b + c
                m, q = f // 4, f % 4
                if m not in received:
                    at = v * CHORD_V + m
                    received[m] = sided(ec, rce[at], rco[at])
                edge = open_chord(*received[m], q, i)
                points = line_points(0, f)
                parts = even_odd(
                    [visc[p] * (gc[v, p] + weights[k] * edge) for k, p in enumerate(points)]
                )
                total, diff = neighbours_chord(*traces(parts), -1.0, i)
                plane.update(zip(points, slope(parts, total, diff)))
            for a in range(5):
                points = line_points(1, 5 * a + c)
                parts = even_odd([fs[v, p] for p in points])
                total, diff = neighbours_span(*traces(parts), is_low, sign_row)
                for p, value in zip(points, slope(parts, total, diff)):
                    res[v, p] = plane[p] + value

        for f in range(NF):
            ends = traces(even_odd([state[v, p] for p in line_points(2, f)]))
            total_ref[f], diff_ref[f] = neighbours_normal(*ends, 1.0, lane)
        across(0)
        across(1)
        for f in range(NF):
            points = line_points(2, f)
            parts = even_odd([state[v, p] for p in points])
            values = slope(parts, total_ref[f], diff_ref[f])
            values = [visc[p] * value for p, value in zip(points, values)]
            for p, value in zip(points, values):
                flux[p] = value
            ends = traces(even_odd(values))
            total_ref[NF + f], diff_ref[NF + f] = neighbours_normal(*ends, -1.0, lane)
        across(2)
        across(3)
        across(4)
        for f in range(NF):
            points = line_points(2, f)
            parts = even_odd([flux[p] for p in points])
            values = slope(parts, total_ref[NF + f], diff_ref[NF + f])
            for p, value in zip(points, values):
                res[v, p] = res[v, p] + value
        return carry

    lax.fori_loop(0, NV, one, 0)
    write.wait()


def close_chord_kernel(res, ce, co, rbce, rbco, out):
    i, _ = row_ids()
    ec = even_chord()
    weights = chord_weights(i)

    def one(v, carry):
        for m in range(CHORD_V):
            at = v * CHORD_V + m
            behind, ahead = sided(
                ec,
                rbce[at] + rbce[CHORD_N + m] * ce[at],
                rbco[at] + rbco[CHORD_N + m] * co[at],
            )
            for f in range(4 * m, min(4 * m + 4, NF)):
                edge = open_chord(behind, ahead, f % 4, i)
                for k, p in enumerate(line_points(0, f)):
                    out[v, p] = res[v, p] + weights[k] * edge
        return carry

    lax.fori_loop(0, NV, one, 0)


def close_span_kernel(res, rbse, rbso, final, edge, out, sems):
    _, j = row_ids()
    is_low = j == 0
    es = even_span()
    weights = span_weights(is_low)

    def send(v):
        return pltpu.make_async_copy(out.at[v], final.at[v], sems.at[v])

    def one(v, carry):
        for m in range(SPAN_V):
            first, second = rbse[v * SPAN_V + m], rbso[v * SPAN_V + m]
            behind, ahead = jnp.where(es, second, first), jnp.where(es, first, second)
            for f in range(2 * m, min(2 * m + 2, NF)):
                edge[f] = open_span(behind, ahead, f % 2, is_low)
        for f in range(NF):
            for k, p in enumerate(line_points(1, f)):
                out[v, p] = res[v, p] + weights[k] * edge[f]

        @pl.when(v > 0)
        def _():
            send(v - 1).start()

        return carry

    lax.fori_loop(0, NV, one, 0)
    send(NV - 1).start()
    for v in range(NV):
        send(v).wait()


def span_weights(is_low):
    return [jnp.where(is_low, float(0.5 * CORR_L[k]), float(0.5 * CORR_R[k])) for k in range(5)]


def chord_weights(i):
    first, last = chord_ends()
    low, high = jnp.logical_and(i == 0, ~first), jnp.logical_and(i == 3, ~last)
    return [
        jnp.where(low, float(0.5 * CORR_L[k]), jnp.where(high, float(0.5 * CORR_R[k]), 0.0))
        for k in range(5)
    ]


def held(*lead):
    return pltpu.VMEM(lead + (ROWS, LANES), jnp.float32)


def vec(*lead):
    return jax.ShapeDtypeStruct(lead + (ROWS, LANES), jnp.float32)


def call(kernel, outs, args, scratch=(), cycles=1000, far_in=(), far_out=(), grant=24 * 2**20):
    vmem, hbm = (pl.BlockSpec(memory_space=m) for m in (pltpu.VMEM, pltpu.HBM))
    total = sum(int(np.prod(x.shape)) for x in list(outs) + list(args)) * 4
    return pl.pallas_call(
        kernel,
        out_shape=outs,
        in_specs=[hbm if n in far_in else vmem for n in range(len(args))],
        out_specs=[hbm if n in far_out else vmem for n in range(len(outs))],
        scratch_shapes=list(scratch),
        compiler_params=pltpu.CompilerParams(vmem_limit_bytes=grant),
        cost_estimate=pl.CostEstimate(flops=cycles * 4096, bytes_accessed=total, transcendentals=0),
    )(*args)


def paired(n, odd, wraps):
    route = []
    for lower in range(odd, n, 2):
        upper = lower + 1
        if upper >= n:
            if not wraps:
                continue
            upper %= n
        route += [(lower, upper), (upper, lower)]
    return route


def shards(state):
    chords, spans = lax.axis_size("chord"), lax.axis_size("span")

    def span_swap(array, odd):
        return lax.ppermute(array, "span", paired(spans, odd, True))

    def chord_swap(array, odd):
        route = [
            (a * spans + c, b * spans + c) for a, b in paired(chords, odd, False) for c in range(spans)
        ]
        if odd:
            route += [
                (a * spans + c, a * spans + (c ^ 1)) for a in (0, chords - 1) for c in range(spans)
            ]
        return lax.ppermute(array, ("chord", "span"), route)

    dma = pltpu.SemaphoreType.DMA
    u = state.reshape(NV, 125, ROWS, LANES)
    (eps,) = call(
        sensor_kernel,
        [vec()],
        [pltpu.with_memory_space_constraint(u, pltpu.HBM)],
        [held(125), held(125), dma(())],
        far_in=(0,),
    )
    rkco = chord_swap(eps, 1)
    rkce = chord_swap(eps, 0)
    so, se = call(leave_span_kernel, [vec(SPAN_N), vec(SPAN_N)], [u])
    rso = span_swap(so, 1)
    co, ce, se, three = call(
        leave_chord_kernel,
        [vec(CHORD_N), vec(CHORD_N), vec(SPAN_N + 3), vec(3)],
        [u, eps, rkce, rkco, se],
    )
    rse = span_swap(se, 0)
    rkso = span_swap(three, 1)
    rco = chord_swap(co, 1)
    gc, gs = call(gradient_kernel, [vec(NV, 125)] * 2, [u], cycles=4000)
    visc, bco, bce = call(
        chord_send_kernel,
        [vec(125), vec(CHORD_N + CHORD_V), vec(CHORD_N + CHORD_V)],
        [gc, three, rkso, rse],
        cycles=2000,
    )
    rbco = chord_swap(bco, 1)
    fs, bso, bse = call(
        span_flux_kernel,
        [vec(NV, 125), vec(SPAN_N), vec(SPAN_N)],
        [gs, visc, rse, rso],
        cycles=2000,
    )
    rbso = span_swap(bso, 1)
    rbce = chord_swap(bce, 0)
    rce = chord_swap(ce, 0)
    rbse = span_swap(bse, 0)
    res, visc_out = call(
        inner_kernel,
        [vec(NV, 125), vec(125)],
        [u, visc, fs, gc, rce, rco],
        [held(2 * NF), held(2 * NF), held(125), dma(())],
        cycles=6000,
        far_out=(1,),
    )
    (res,) = call(close_chord_kernel, [vec(NV, 125)], [res, ce, co, rbce, rbco], cycles=1000)
    (out,) = call(
        close_span_kernel,
        [vec(NV, 125)],
        [res, rbse, rbso],
        [held(NF), held(NV, 125), dma((NV,))],
        cycles=2000,
        far_out=(0,),
    )
    return (out.reshape(state.shape), visc_out.reshape(state.shape[1:]))


def solution(mesh):
    in_specs = (P(None, None, "chord", "span", None),)
    out_specs = (P(None, None, "chord", "span", None), P(None, "chord", "span", None))

    return jax.shard_map(shards, mesh=mesh, in_specs=in_specs, out_specs=out_specs, check_vma=False)
```

```python
import math

import jax
import jax.numpy as jnp
import numpy as np
from jax import lax
from jax.experimental import pallas as pl
from jax.experimental.pallas import tpu as pltpu
from jax.sharding import PartitionSpec as P


EPS_SCALE = 0.01
SENSOR_CENTRE = -3.0
SENSOR_WIDTH = 1.5
RATIO_FLOOR = 1e-06
ENERGY_EPS = 1e-06
GAUSS_NODES = [-0.906179845938664, -0.5384693101056831, 0.0, 0.5384693101056831, 0.906179845938664]
GAUSS_WEIGHTS = [
    0.2369268850561891,
    0.4786286704993665,
    0.5688888888888889,
    0.4786286704993665,
    0.2369268850561891,
]


def legendre_values(points):
    values = [np.ones(points.shape), np.array(points)]
    for order in range(1, 5):
        values.append(
            ((2 * order + 1) * points * values[order] - order * values[order - 1]) / (order + 1)
        )
    return values


def line_tables():
    line_nodes = np.array(GAUSS_NODES)
    quadrature_weights = np.array(GAUSS_WEIGHTS)
    barycentric = np.array(
        [
            1.0 / np.prod([line_nodes[j] - line_nodes[k] for k in range(5) if k != j])
            for j in range(5)
        ]
    )
    derivative = np.zeros((5, 5))
    for i in range(5):
        for j in range(5):
            if i != j:
                derivative[i, j] = barycentric[j] / barycentric[i] / (line_nodes[i] - line_nodes[j])
        derivative[i, i] = -np.sum(derivative[i])
    left_values = np.ones(5)
    right_values = np.ones(5)
    for j in range(5):
        for k in range(5):
            if k != j:
                left_values[j] *= (-1.0 - line_nodes[k]) / (line_nodes[j] - line_nodes[k])
                right_values[j] *= (1.0 - line_nodes[k]) / (line_nodes[j] - line_nodes[k])
    legendre = legendre_values(line_nodes)
    fourth_slope = 7.0 * legendre[3] + 3.0 * legendre[1]
    fifth_slope = 9.0 * legendre[4] + 5.0 * legendre[2] + legendre[0]
    modal = np.zeros((5, 5))
    for k in range(5):
        modal[k, :] = quadrature_weights * math.sqrt((2 * k + 1) / 2.0) * legendre[k]
    return (line_nodes, derivative, left_values, right_values, fourth_slope, fifth_slope, modal)


NODES, DERIV, LEFT, RIGHT, SLOPE4, SLOPE5, MODAL = line_tables()
CORR_L = 0.5 * (SLOPE4 - SLOPE5)
CORR_R = 0.5 * (SLOPE4 + SLOPE5)
OWN = DERIV - 0.5 * (np.outer(CORR_L, LEFT) + np.outer(CORR_R, RIGHT))
ROWS, LANES = 8, 128
NV, NF = 5, 25
SPAN_V, CHORD_V = 13, 7
SPAN_N, CHORD_N = NV * SPAN_V, NV * CHORD_V


def mul(scale, x):
    return float(scale) * x


def even_odd(x):
    return (x[0] + x[4], x[1] + x[3], x[0] - x[4], x[1] - x[3], x[2])


def traces(parts):
    e0, e1, o0, o1, c = parts
    even = (
        mul(0.5 * (LEFT[0] + LEFT[4]), e0) + mul(0.5 * (LEFT[1] + LEFT[3]), e1) + mul(LEFT[2], c)
    )
    odd = mul(0.5 * (LEFT[0] - LEFT[4]), o0) + mul(0.5 * (LEFT[1] - LEFT[3]), o1)
    return (even + odd, even - odd)


def slope(parts, total, diff):
    e0, e1, o0, o1, c = parts
    even, odd = [], []
    for i in range(3):
        even.append(
            mul(0.5 * (OWN[i, 0] - OWN[i, 4]), o0)
            + mul(0.5 * (OWN[i, 1] - OWN[i, 3]), o1)
            + mul(0.25 * SLOPE5[i], diff)
        )
    for i in range(2):
        odd.append(
            mul(0.5 * (OWN[i, 0] + OWN[i, 4]), e0)
            + mul(0.5 * (OWN[i, 1] + OWN[i, 3]), e1)
            + (mul(OWN[i, 2], c) + mul(0.25 * SLOPE4[i], total))
        )
    return [
        even[0] + odd[0],
        even[1] + odd[1],
        even[2],
        even[1] - odd[1],
        even[0] - odd[0],
    ]


def modal_line(x):
    e0, e1, o0, o1, c = even_odd(x)
    out = []
    for k in range(5):
        if k % 2 == 0:
            out.append(mul(MODAL[k, 0], e0) + mul(MODAL[k, 1], e1) + mul(MODAL[k, 2], c))
        else:
            out.append(mul(MODAL[k, 0], o0) + mul(MODAL[k, 1], o1))
    return out


def line_points(axis, f):
    a, b = f // 5, f % 5
    if axis == 0:
        return [25 * k + 5 * a + b for k in range(5)]
    if axis == 1:
        return [25 * a + 5 * k + b for k in range(5)]
    return [25 * a + 5 * b + k for k in range(5)]


def row_ids():
    rows = lax.broadcasted_iota(jnp.int32, (ROWS, LANES), 0)
    return (rows // 2, rows % 2)


def lane_ids():
    return lax.broadcasted_iota(jnp.int32, (ROWS, LANES), 1)


def up_rows(x, n):
    n = n % ROWS
    return x if n == 0 else pltpu.roll(x, n, 0)


def splat_flag(flag):
    return jnp.full((ROWS, LANES), flag.astype(jnp.int32), jnp.int32) > 0


def chord_ends():
    at = lax.axis_index("chord")
    return (splat_flag(at == 0), splat_flag(at == lax.axis_size("chord") - 1))


def even_span():
    return splat_flag(lax.axis_index("span") % 2 == 0)


def even_chord():
    return splat_flag(lax.axis_index("chord") % 2 == 0)


def pack_span(out_of, is_low, even, first_ref, second_ref, base, count=NF):
    for m in range((count + 1) // 2):
        f0 = out_of(2 * m)
        f1 = out_of(2 * m + 1) if 2 * m + 1 < count else f0
        up = jnp.where(is_low, up_rows(f0, -1), f1)
        down = jnp.where(is_low, f0, up_rows(f1, 1))
        first_ref[base + m] = jnp.where(even, up, down)
        second_ref[base + m] = jnp.where(even, down, up)


def pack_chord(out_of, i, even, first_ref, second_ref, base, count=NF):
    for m in range((count + 3) // 4):
        up = down = None
        for q in range(4):
            f = 4 * m + q
            if f >= count:
                continue
            trace = out_of(f)
            u, d = up_rows(trace, 2 * q - 6), up_rows(trace, 2 * q)
            up = u if up is None else jnp.where(i == q, u, up)
            down = d if down is None else jnp.where(i == q, d, down)
        first_ref[base + m] = jnp.where(even, up, down)
        second_ref[base + m] = jnp.where(even, down, up)


def open_span(below, above, q, is_low):
    if q == 0:
        return jnp.where(is_low, below, up_rows(above, 1))
    return jnp.where(is_low, up_rows(below, -1), above)


def open_chord(below, above, q, i):
    return jnp.where(i == 0, up_rows(below, -2 * q), up_rows(above, 6 - 2 * q))


def sided(even, first, second):
    return (jnp.where(even, second, first), jnp.where(even, first, second))


def sensor_kernel(source, eps, density, work, sem):
    read = pltpu.make_async_copy(source.at[0], density, sem)
    read.start()
    read.wait()
    eps[...] = sensor(density, work)


def leave_chord_kernel(state, co, ce):
    i, _ = row_ids()
    first_row = i == 0
    ec = even_chord()

    def one(v, carry):
        def leaving(f):
            left, right = traces(even_odd([state[v, p] for p in line_points(0, f)]))
            return jnp.where(first_row, left, right)

        pack_chord(leaving, i, ec, ce, co, v * CHORD_V)
        return carry

    lax.fori_loop(0, NV, one, 0)


def three_kernel(eps, rkce, rkco, traces_even, three, se):
    first, last = chord_ends()
    behind, ahead = sided(even_chord(), rkce[...], rkco[...])
    three[0] = eps[...]
    three[1] = jnp.where(first, 0.0, behind)
    three[2] = jnp.where(last, 0.0, ahead)
    for n in range(3):
        se[SPAN_N + n] = three[n]
    for m in range(SPAN_N):
        se[m] = traces_even[m]


def leave_span_kernel(state, so, se):
    _, j = row_ids()
    is_low = j == 0
    es = even_span()

    def one(v, carry):
        def leaving(f):
            left, right = traces(even_odd([state[v, p] for p in line_points(1, f)]))
            return jnp.where(is_low, left, right)

        pack_span(leaving, is_low, es, se, so, v * SPAN_V)
        return carry

    lax.fori_loop(0, NV, one, 0)


def sensor(density, work):
    for axis in range(2):
        origin = density if axis == 0 else work
        for f in range(NF):
            points = line_points(axis, f)
            for p, value in zip(points, modal_line([origin[p] for p in points])):
                work[p] = value
    low_sums, high_sums = [], []
    for f in range(NF):
        a, b = f // 5, f % 5
        low, high = None, None
        for k, value in enumerate(modal_line([work[p] for p in line_points(2, f)])):
            square = value * value
            if a == 4 or b == 4 or k == 4:
                high = square if high is None else high + square
            else:
                low = square if low is None else low + square
        if low is not None:
            low_sums.append(low)
        high_sums.append(high)

    def tree(values):
        while len(values) > 1:
            values = [
                values[n] + values[n + 1] if n + 1 < len(values) else values[n]
                for n in range(0, len(values), 2)
            ]
        return values[0]

    high_part = tree(high_sums)
    total = (tree(low_sums) + high_part) + ENERGY_EPS
    level = jnp.log(jnp.maximum(high_part / total, RATIO_FLOOR)) * (1.0 / math.log(10.0))
    ramp = jnp.clip((level - SENSOR_CENTRE) / SENSOR_WIDTH, -1.0, 1.0)
    eps = EPS_SCALE * 0.5 * (1.0 + jnp.sin(0.5 * math.pi * ramp))
    return eps


def neighbours_chord(left, right, sign, i):
    first = (lax.axis_index("chord") == 0).astype(jnp.float32) * sign
    last = (lax.axis_index("chord") == lax.axis_size("chord") - 1).astype(jnp.float32) * sign
    before = jnp.where(i == 0, left * first, up_rows(right, 2))
    after = jnp.where(i == 3, right * last, up_rows(left, -2))
    return (before + after, after - before)


def neighbours_span(left, right, is_low, sign_row):
    inner = jnp.where(is_low, up_rows(left, -1), up_rows(right, 1))
    return (inner, inner * sign_row)


def neighbours_normal(left, right, sign, lane):
    before = jnp.where(lane == 0, mul(sign, left), pltpu.roll(right, 1, 1))
    after = jnp.where(lane == LANES - 1, mul(sign, right), pltpu.roll(left, LANES - 1, 1))
    return (before + after, after - before)


def gradient_kernel(state, gc, gs):
    i, j = row_ids()
    is_low = j == 0
    sign_row = jnp.where(is_low, 1.0, -1.0)

    def one(v, carry):
        for axis, ref in ((0, gc), (1, gs)):
            for f in range(NF):
                points = line_points(axis, f)
                parts = even_odd([state[v, p] for p in points])
                left, right = traces(parts)
                if axis == 0:
                    total, diff = neighbours_chord(left, right, 1.0, i)
                else:
                    total, diff = neighbours_span(left, right, is_low, sign_row)
                for p, value in zip(points, slope(parts, total, diff)):
                    ref[v, p] = value
        return carry

    lax.fori_loop(0, NV, one, 0)


def viscosity_into(visc, own, behind, ahead):
    i, j = row_ids()
    lane = lane_ids()
    is_low = j == 0

    def chord_pair(mid, low, high):
        under = up_rows(jnp.where(i == 3, low, mid), 2)
        over = up_rows(jnp.where(i == 0, high, mid), -2)
        return (jnp.maximum(mid, under), jnp.maximum(mid, over))

    mids, befores, afters = (chord_pair(own[n], behind[n], ahead[n]) for n in range(3))
    corners = {}
    for x in range(2):
        mid, low, high = mids[x], befores[x], afters[x]
        under = jnp.where(is_low, up_rows(low, -1), up_rows(mid, 1))
        over = jnp.where(is_low, up_rows(mid, -1), up_rows(high, 1))
        for y, value in enumerate((jnp.maximum(mid, under), jnp.maximum(mid, over))):
            low_z = jnp.where(lane == 0, value, pltpu.roll(value, 1, 1))
            high_z = jnp.where(lane == LANES - 1, value, pltpu.roll(value, LANES - 1, 1))
            corners[x, y, 0] = jnp.maximum(value, low_z)
            corners[x, y, 1] = jnp.maximum(value, high_z)
    halves = [((1.0 - x) / 2.0, (1.0 + x) / 2.0) for x in NODES]
    for a in range(5):
        plane = {
            (y, z): mul(halves[a][0], corners[0, y, z]) + mul(halves[a][1], corners[1, y, z])
            for y in range(2)
            for z in range(2)
        }
        for b in range(5):
            low, high = (
                mul(halves[b][0], plane[0, z]) + mul(halves[b][1], plane[1, z]) for z in range(2)
            )
            for c in range(5):
                visc[25 * a + 5 * b + c] = mul(halves[c][0], low) + mul(halves[c][1], high)
    return corners


SHARE = 0.5 * LEFT * CORR_L
SHARE_FAR = float(np.sum(SHARE * (1.0 + NODES) / 2.0))
SHARE_NEAR = float(np.sum(SHARE * (1.0 - NODES) / 2.0))


def chord_send_kernel(gc, three, rkso, rse, visc, bco, bce, near):
    i, _ = row_ids()
    first_row = i == 0
    es, ec = even_span(), even_chord()
    corners = viscosity_into(
        visc, *((three[n],) + sided(es, rse[SPAN_N + n], rkso[n]) for n in range(3))
    )
    for n in range(4):
        y, z = n // 2, n % 2
        near[n] = SHARE_NEAR * jnp.where(first_row, -corners[0, y, z], corners[1, y, z])

    def far(n):
        return jnp.where(first_row, corners[1, n // 2, n % 2], corners[0, n // 2, n % 2])

    pack_chord(far, i, ec, bce, bco, CHORD_N, 4)

    def one(v, carry):
        def leaving(f):
            left, right = traces(even_odd([visc[p] * gc[v, p] for p in line_points(0, f)]))
            return jnp.where(first_row, left, right)

        pack_chord(leaving, i, ec, bce, bco, v * CHORD_V)
        return carry

    lax.fori_loop(0, NV, one, 0)


def span_flux_kernel(gs, visc, rse, rso, fs, bso, bse):
    _, j = row_ids()
    is_low = j == 0
    es = even_span()
    weights = span_weights(is_low)

    def one(v, carry):
        received = {}

        def leaving(f):
            m, q = f // 2, f % 2
            if m not in received:
                base = v * SPAN_V + m
                received[m] = sided(es, rse[base], rso[base])
            edge = open_span(received[m][0], received[m][1], q, is_low)
            values = []
            for k, p in enumerate(line_points(1, f)):
                value = visc[p] * (gs[v, p] + weights[k] * edge)
                fs[v, p] = value
                values.append(value)
            left, right = traces(even_odd(values))
            return jnp.where(is_low, left, right)

        pack_span(leaving, is_low, es, bse, bso, v * SPAN_V)
        return carry

    lax.fori_loop(0, NV, one, 0)


def factors_into(factor, far, near, behind_row):
    value = [
        jnp.where(behind_row, -SHARE_FAR, SHARE_FAR) * far[n] + near[n] for n in range(4)
    ]
    halves = [((1.0 - x) / 2.0, (1.0 + x) / 2.0) for x in NODES]
    for a in range(5):
        low, high = (
            mul(halves[a][0], value[z]) + mul(halves[a][1], value[2 + z]) for z in range(2)
        )
        for c in range(5):
            factor[5 * a + c] = mul(halves[c][0], low) + mul(halves[c][1], high)


def inner_kernel(state, visc, fs, gc, rce, rco, res, visc_out, total_ref, diff_ref, flux, sem):
    write = pltpu.make_async_copy(visc, visc_out, sem)
    write.start()
    i, j = row_ids()
    lane = lane_ids()
    is_low = j == 0
    sign_row = jnp.where(is_low, 1.0, -1.0)
    ec = even_chord()
    weights = chord_weights(i)

    def one(v, carry):
        received = {}

        def across(c):
            plane = {}
            for b in range(5):
                f = 5 * b + c
                m, q = f // 4, f % 4
                if m not in received:
                    at = v * CHORD_V + m
                    received[m] = sided(ec, rce[at], rco[at])
                edge = open_chord(*received[m], q, i)
                points = line_points(0, f)
                parts = even_odd(
                    [visc[p] * (gc[v, p] + weights[k] * edge) for k, p in enumerate(points)]
                )
                total, diff = neighbours_chord(*traces(parts), -1.0, i)
                plane.update(zip(points, slope(parts, total, diff)))
            for a in range(5):
                points = line_points(1, 5 * a + c)
                parts = even_odd([fs[v, p] for p in points])
                total, diff = neighbours_span(*traces(parts), is_low, sign_row)
                for p, value in zip(points, slope(parts, total, diff)):
                    res[v, p] = plane[p] + value

        for f in range(NF):
            ends = traces(even_odd([state[v, p] for p in line_points(2, f)]))
            total_ref[f], diff_ref[f] = neighbours_normal(*ends, 1.0, lane)
        across(0)
        across(1)
        for f in range(NF):
            points = line_points(2, f)
            parts = even_odd([state[v, p] for p in points])
            values = slope(parts, total_ref[f], diff_ref[f])
            values = [visc[p] * value for p, value in zip(points, values)]
            for p, value in zip(points, values):
                flux[p] = value
            ends = traces(even_odd(values))
            total_ref[NF + f], diff_ref[NF + f] = neighbours_normal(*ends, -1.0, lane)
        across(2)
        across(3)
        across(4)
        for f in range(NF):
            points = line_points(2, f)
            parts = even_odd([flux[p] for p in points])
            values = slope(parts, total_ref[NF + f], diff_ref[NF + f])
            for p, value in zip(points, values):
                res[v, p] = res[v, p] + value
        return carry

    lax.fori_loop(0, NV, one, 0)
    write.wait()


def close_chord_kernel(res, ce, co, rbce, rbco, near, out, factor):
    i, _ = row_ids()
    ec = even_chord()
    weights = chord_weights(i)
    far = sided(ec, rbce[CHORD_N], rbco[CHORD_N])
    factors_into(factor, [open_chord(*far, n, i) for n in range(4)], near, i == 0)

    def one(v, carry):
        for m in range(CHORD_V):
            at = v * CHORD_V + m
            received, own = sided(ec, rbce[at], rbco[at]), sided(ec, ce[at], co[at])
            for f in range(4 * m, min(4 * m + 4, NF)):
                q = f % 4
                edge = open_chord(*received, q, i) + factor[f] * open_chord(*own, q, i)
                for k, p in enumerate(line_points(0, f)):
                    out[v, p] = res[v, p] + weights[k] * edge
        return carry

    lax.fori_loop(0, NV, one, 0)


def close_span_kernel(res, rbse, rbso, final, out, sems):
    _, j = row_ids()
    is_low = j == 0
    es = even_span()
    weights = span_weights(is_low)

    def send(v, a):
        points = pl.ds(NF * a, NF)
        return pltpu.make_async_copy(out.at[v, points], final.at[v, points], sems.at[v, a])

    def one(v, carry):
        for m in range(SPAN_V):
            first, second = rbse[v * SPAN_V + m], rbso[v * SPAN_V + m]
            behind, ahead = jnp.where(es, second, first), jnp.where(es, first, second)
            for f in range(2 * m, min(2 * m + 2, NF)):
                edge = open_span(behind, ahead, f % 2, is_low)
                for k, p in enumerate(line_points(1, f)):
                    out[v, p] = res[v, p] + weights[k] * edge
                a, c = f // 5, f % 5
                if c == 4 and a > 0:
                    send(v, a - 1).start()
                elif c == 4:

                    @pl.when(v > 0)
                    def _():
                        send(v - 1, 4).start()

        return carry

    lax.fori_loop(0, NV, one, 0)
    send(NV - 1, 4).start()
    for v in range(NV):
        for a in range(5):
            send(v, a).wait()


def span_weights(is_low):
    return [jnp.where(is_low, float(0.5 * CORR_L[k]), float(0.5 * CORR_R[k])) for k in range(5)]


def chord_weights(i):
    first, last = chord_ends()
    low, high = jnp.logical_and(i == 0, ~first), jnp.logical_and(i == 3, ~last)
    return [
        jnp.where(low, float(0.5 * CORR_L[k]), jnp.where(high, float(0.5 * CORR_R[k]), 0.0))
        for k in range(5)
    ]


def held(*lead):
    return pltpu.VMEM(lead + (ROWS, LANES), jnp.float32)


def vec(*lead):
    return jax.ShapeDtypeStruct(lead + (ROWS, LANES), jnp.float32)


def call(kernel, outs, args, scratch=(), cycles=1000, far_in=(), far_out=(), grant=24 * 2**20):
    vmem, hbm = (pl.BlockSpec(memory_space=m) for m in (pltpu.VMEM, pltpu.HBM))
    total = sum(int(np.prod(x.shape)) for x in list(outs) + list(args)) * 4
    return pl.pallas_call(
        kernel,
        out_shape=outs,
        in_specs=[hbm if n in far_in else vmem for n in range(len(args))],
        out_specs=[hbm if n in far_out else vmem for n in range(len(outs))],
        scratch_shapes=list(scratch),
        compiler_params=pltpu.CompilerParams(vmem_limit_bytes=grant),
        cost_estimate=pl.CostEstimate(flops=cycles * 4096, bytes_accessed=total, transcendentals=0),
    )(*args)


def paired(n, odd, wraps):
    route = []
    for lower in range(odd, n, 2):
        upper = lower + 1
        if upper >= n:
            if not wraps:
                continue
            upper %= n
        route += [(lower, upper), (upper, lower)]
    return route


def shards(state):
    chords, spans = lax.axis_size("chord"), lax.axis_size("span")

    def span_swap(array, odd):
        return lax.ppermute(array, "span", paired(spans, odd, True))

    def chord_swap(array, odd):
        route = [
            (a * spans + c, b * spans + c) for a, b in paired(chords, odd, False) for c in range(spans)
        ]
        if odd:
            route += [
                (a * spans + c, a * spans + (c ^ 1)) for a in (0, chords - 1) for c in range(spans)
            ]
        return lax.ppermute(array, ("chord", "span"), route)

    dma = pltpu.SemaphoreType.DMA
    u = state.reshape(NV, 125, ROWS, LANES)
    (eps,) = call(
        sensor_kernel,
        [vec()],
        [pltpu.with_memory_space_constraint(u, pltpu.HBM)],
        [held(125), held(125), dma(())],
        far_in=(0,),
    )
    rkco = chord_swap(eps, 1)
    rkce = chord_swap(eps, 0)
    so, se = call(leave_span_kernel, [vec(SPAN_N), vec(SPAN_N)], [u])
    rso = span_swap(so, 1)
    three, se = call(three_kernel, [vec(3), vec(SPAN_N + 3)], [eps, rkce, rkco, se], cycles=100)
    rkso = span_swap(three, 1)
    co, ce = call(leave_chord_kernel, [vec(CHORD_N), vec(CHORD_N)], [u])
    rco = chord_swap(co, 1)
    rce = chord_swap(ce, 0)
    rse = span_swap(se, 0)
    gc, gs = call(gradient_kernel, [vec(NV, 125)] * 2, [u], cycles=4000)
    visc, bco, bce, near = call(
        chord_send_kernel,
        [vec(125), vec(CHORD_N + 1), vec(CHORD_N + 1), vec(4)],
        [gc, three, rkso, rse],
        cycles=2000,
    )
    rbco = chord_swap(bco, 1)
    fs, bso, bse = call(
        span_flux_kernel,
        [vec(NV, 125), vec(SPAN_N), vec(SPAN_N)],
        [gs, visc, rse, rso],
        cycles=2000,
    )
    rbso = span_swap(bso, 1)
    rbce = chord_swap(bce, 0)
    rbse = span_swap(bse, 0)
    res, visc_out = call(
        inner_kernel,
        [vec(NV, 125), vec(125)],
        [u, visc, fs, gc, rce, rco],
        [held(2 * NF), held(2 * NF), held(125), dma(())],
        cycles=8000,
        far_out=(1,),
    )
    (res,) = call(
        close_chord_kernel, [vec(NV, 125)], [res, ce, co, rbce, rbco, near], [held(NF)], cycles=1000
    )
    (out,) = call(
        close_span_kernel,
        [vec(NV, 125)],
        [res, rbse, rbso],
        [held(NV, 125), dma((NV, 5))],
        cycles=2000,
        far_out=(0,),
    )
    return (out.reshape(state.shape), visc_out.reshape(state.shape[1:]))


def solution(mesh):
    in_specs = (P(None, None, "chord", "span", None),)
    out_specs = (P(None, None, "chord", "span", None), P(None, "chord", "span", None))

    return jax.shard_map(shards, mesh=mesh, in_specs=in_specs, out_specs=out_specs, check_vma=False)
```

```python
import math

import jax
import jax.numpy as jnp
import numpy as np
from jax import lax
from jax.experimental import pallas as pl
from jax.experimental.pallas import tpu as pltpu
from jax.sharding import PartitionSpec as P


EPS_SCALE = 0.01
SENSOR_CENTRE = -3.0
SENSOR_WIDTH = 1.5
RATIO_FLOOR = 1e-06
ENERGY_EPS = 1e-06
GAUSS_NODES = [-0.906179845938664, -0.5384693101056831, 0.0, 0.5384693101056831, 0.906179845938664]
GAUSS_WEIGHTS = [
    0.2369268850561891,
    0.4786286704993665,
    0.5688888888888889,
    0.4786286704993665,
    0.2369268850561891,
]


def legendre_values(points):
    values = [np.ones(points.shape), np.array(points)]
    for order in range(1, 5):
        values.append(
            ((2 * order + 1) * points * values[order] - order * values[order - 1]) / (order + 1)
        )
    return values


def line_tables():
    line_nodes = np.array(GAUSS_NODES)
    quadrature_weights = np.array(GAUSS_WEIGHTS)
    barycentric = np.array(
        [
            1.0 / np.prod([line_nodes[j] - line_nodes[k] for k in range(5) if k != j])
            for j in range(5)
        ]
    )
    derivative = np.zeros((5, 5))
    for i in range(5):
        for j in range(5):
            if i != j:
                derivative[i, j] = barycentric[j] / barycentric[i] / (line_nodes[i] - line_nodes[j])
        derivative[i, i] = -np.sum(derivative[i])
    left_values = np.ones(5)
    right_values = np.ones(5)
    for j in range(5):
        for k in range(5):
            if k != j:
                left_values[j] *= (-1.0 - line_nodes[k]) / (line_nodes[j] - line_nodes[k])
                right_values[j] *= (1.0 - line_nodes[k]) / (line_nodes[j] - line_nodes[k])
    legendre = legendre_values(line_nodes)
    fourth_slope = 7.0 * legendre[3] + 3.0 * legendre[1]
    fifth_slope = 9.0 * legendre[4] + 5.0 * legendre[2] + legendre[0]
    modal = np.zeros((5, 5))
    for k in range(5):
        modal[k, :] = quadrature_weights * math.sqrt((2 * k + 1) / 2.0) * legendre[k]
    return (line_nodes, derivative, left_values, right_values, fourth_slope, fifth_slope, modal)


NODES, DERIV, LEFT, RIGHT, SLOPE4, SLOPE5, MODAL = line_tables()
CORR_L = 0.5 * (SLOPE4 - SLOPE5)
CORR_R = 0.5 * (SLOPE4 + SLOPE5)
OWN = DERIV - 0.5 * (np.outer(CORR_L, LEFT) + np.outer(CORR_R, RIGHT))
ROWS, LANES = 8, 128
NV, NF = 5, 25
SPAN_V, CHORD_V = 13, 7
SPAN_N, CHORD_N = NV * SPAN_V, NV * CHORD_V


def mul(scale, x):
    return float(scale) * x


def even_odd(x):
    return (x[0] + x[4], x[1] + x[3], x[0] - x[4], x[1] - x[3], x[2])


def traces(parts):
    e0, e1, o0, o1, c = parts
    even = (
        mul(0.5 * (LEFT[0] + LEFT[4]), e0) + mul(0.5 * (LEFT[1] + LEFT[3]), e1) + mul(LEFT[2], c)
    )
    odd = mul(0.5 * (LEFT[0] - LEFT[4]), o0) + mul(0.5 * (LEFT[1] - LEFT[3]), o1)
    return (even + odd, even - odd)


def slope(parts, total, diff):
    e0, e1, o0, o1, c = parts
    even, odd = [], []
    for i in range(3):
        even.append(
            mul(0.5 * (OWN[i, 0] - OWN[i, 4]), o0)
            + mul(0.5 * (OWN[i, 1] - OWN[i, 3]), o1)
            + mul(0.25 * SLOPE5[i], diff)
        )
    for i in range(2):
        odd.append(
            mul(0.5 * (OWN[i, 0] + OWN[i, 4]), e0)
            + mul(0.5 * (OWN[i, 1] + OWN[i, 3]), e1)
            + (mul(OWN[i, 2], c) + mul(0.25 * SLOPE4[i], total))
        )
    return [
        even[0] + odd[0],
        even[1] + odd[1],
        even[2],
        even[1] - odd[1],
        even[0] - odd[0],
    ]


def modal_line(x):
    e0, e1, o0, o1, c = even_odd(x)
    out = []
    for k in range(5):
        if k % 2 == 0:
            out.append(mul(MODAL[k, 0], e0) + mul(MODAL[k, 1], e1) + mul(MODAL[k, 2], c))
        else:
            out.append(mul(MODAL[k, 0], o0) + mul(MODAL[k, 1], o1))
    return out


def line_points(axis, f):
    a, b = f // 5, f % 5
    if axis == 0:
        return [25 * k + 5 * a + b for k in range(5)]
    if axis == 1:
        return [25 * a + 5 * k + b for k in range(5)]
    return [25 * a + 5 * b + k for k in range(5)]


def row_ids():
    rows = lax.broadcasted_iota(jnp.int32, (ROWS, LANES), 0)
    return (rows // 2, rows % 2)


def lane_ids():
    return lax.broadcasted_iota(jnp.int32, (ROWS, LANES), 1)


def up_rows(x, n):
    n = n % ROWS
    return x if n == 0 else pltpu.roll(x, n, 0)


def splat_flag(flag):
    return jnp.full((ROWS, LANES), flag.astype(jnp.int32), jnp.int32) > 0


def chord_ends():
    at = lax.axis_index("chord")
    return (splat_flag(at == 0), splat_flag(at == lax.axis_size("chord") - 1))


def even_span():
    return splat_flag(lax.axis_index("span") % 2 == 0)


def even_chord():
    return splat_flag(lax.axis_index("chord") % 2 == 0)


def pack_span(out_of, is_low, even, first_ref, second_ref, base, count=NF):
    for m in range((count + 1) // 2):
        f0 = out_of(2 * m)
        f1 = out_of(2 * m + 1) if 2 * m + 1 < count else f0
        up = jnp.where(is_low, up_rows(f0, -1), f1)
        down = jnp.where(is_low, f0, up_rows(f1, 1))
        first_ref[base + m] = jnp.where(even, up, down)
        second_ref[base + m] = jnp.where(even, down, up)


def pack_chord(out_of, i, even, first_ref, second_ref, base, count=NF):
    for m in range((count + 3) // 4):
        up = down = None
        for q in range(4):
            f = 4 * m + q
            if f >= count:
                continue
            trace = out_of(f)
            u, d = up_rows(trace, 2 * q - 6), up_rows(trace, 2 * q)
            up = u if up is None else jnp.where(i == q, u, up)
            down = d if down is None else jnp.where(i == q, d, down)
        first_ref[base + m] = jnp.where(even, up, down)
        second_ref[base + m] = jnp.where(even, down, up)


def open_span(below, above, q, is_low):
    if q == 0:
        return jnp.where(is_low, below, up_rows(above, 1))
    return jnp.where(is_low, up_rows(below, -1), above)


def open_chord(below, above, q, i):
    return jnp.where(i == 0, up_rows(below, -2 * q), up_rows(above, 6 - 2 * q))


def sided(even, first, second):
    return (jnp.where(even, second, first), jnp.where(even, first, second))


def sensor_kernel(source, eps, density, work, sem):
    read = pltpu.make_async_copy(source.at[0], density, sem)
    read.start()
    read.wait()
    eps[...] = sensor(density, work)


def leave_chord_kernel(state, co, ce):
    i, _ = row_ids()
    first_row = i == 0
    ec = even_chord()

    def one(v, carry):
        def leaving(f):
            left, right = traces(even_odd([state[v, p] for p in line_points(0, f)]))
            return jnp.where(first_row, left, right)

        pack_chord(leaving, i, ec, ce, co, v * CHORD_V)
        return carry

    lax.fori_loop(0, NV, one, 0)


def three_kernel(eps, rkce, rkco, traces_even, three, se):
    first, last = chord_ends()
    behind, ahead = sided(even_chord(), rkce[...], rkco[...])
    three[0] = eps[...]
    three[1] = jnp.where(first, 0.0, behind)
    three[2] = jnp.where(last, 0.0, ahead)
    for n in range(3):
        se[SPAN_N + n] = three[n]
    for m in range(SPAN_N):
        se[m] = traces_even[m]


def leave_span_kernel(state, so, se):
    _, j = row_ids()
    is_low = j == 0
    es = even_span()

    def one(v, carry):
        def leaving(f):
            left, right = traces(even_odd([state[v, p] for p in line_points(1, f)]))
            return jnp.where(is_low, left, right)

        pack_span(leaving, is_low, es, se, so, v * SPAN_V)
        return carry

    lax.fori_loop(0, NV, one, 0)


def sensor(density, work):
    for axis in range(2):
        origin = density if axis == 0 else work
        for f in range(NF):
            points = line_points(axis, f)
            for p, value in zip(points, modal_line([origin[p] for p in points])):
                work[p] = value
    low_sums, high_sums = [], []
    for f in range(NF):
        a, b = f // 5, f % 5
        low, high = None, None
        for k, value in enumerate(modal_line([work[p] for p in line_points(2, f)])):
            square = value * value
            if a == 4 or b == 4 or k == 4:
                high = square if high is None else high + square
            else:
                low = square if low is None else low + square
        if low is not None:
            low_sums.append(low)
        high_sums.append(high)

    def tree(values):
        while len(values) > 1:
            values = [
                values[n] + values[n + 1] if n + 1 < len(values) else values[n]
                for n in range(0, len(values), 2)
            ]
        return values[0]

    high_part = tree(high_sums)
    total = (tree(low_sums) + high_part) + ENERGY_EPS
    level = jnp.log(jnp.maximum(high_part / total, RATIO_FLOOR)) * (1.0 / math.log(10.0))
    ramp = jnp.clip((level - SENSOR_CENTRE) / SENSOR_WIDTH, -1.0, 1.0)
    eps = EPS_SCALE * 0.5 * (1.0 + jnp.sin(0.5 * math.pi * ramp))
    return eps


def neighbours_chord(left, right, sign, i):
    first = (lax.axis_index("chord") == 0).astype(jnp.float32) * sign
    last = (lax.axis_index("chord") == lax.axis_size("chord") - 1).astype(jnp.float32) * sign
    before = jnp.where(i == 0, left * first, up_rows(right, 2))
    after = jnp.where(i == 3, right * last, up_rows(left, -2))
    return (before + after, after - before)


def neighbours_span(left, right, is_low, sign_row):
    inner = jnp.where(is_low, up_rows(left, -1), up_rows(right, 1))
    return (inner, inner * sign_row)


def neighbours_normal(left, right, sign, lane):
    before = jnp.where(lane == 0, mul(sign, left), pltpu.roll(right, 1, 1))
    after = jnp.where(lane == LANES - 1, mul(sign, right), pltpu.roll(left, LANES - 1, 1))
    return (before + after, after - before)


def gradient_kernel(state, gc, gs):
    i, j = row_ids()
    is_low = j == 0
    sign_row = jnp.where(is_low, 1.0, -1.0)

    def one(v, carry):
        for axis, ref in ((0, gc), (1, gs)):
            for f in range(NF):
                points = line_points(axis, f)
                parts = even_odd([state[v, p] for p in points])
                left, right = traces(parts)
                if axis == 0:
                    total, diff = neighbours_chord(left, right, 1.0, i)
                else:
                    total, diff = neighbours_span(left, right, is_low, sign_row)
                for p, value in zip(points, slope(parts, total, diff)):
                    ref[v, p] = value
        return carry

    lax.fori_loop(0, NV, one, 0)


def viscosity_into(visc, own, behind, ahead):
    i, j = row_ids()
    lane = lane_ids()
    is_low = j == 0

    def chord_pair(mid, low, high):
        under = up_rows(jnp.where(i == 3, low, mid), 2)
        over = up_rows(jnp.where(i == 0, high, mid), -2)
        return (jnp.maximum(mid, under), jnp.maximum(mid, over))

    mids, befores, afters = (chord_pair(own[n], behind[n], ahead[n]) for n in range(3))
    corners = {}
    for x in range(2):
        mid, low, high = mids[x], befores[x], afters[x]
        under = jnp.where(is_low, up_rows(low, -1), up_rows(mid, 1))
        over = jnp.where(is_low, up_rows(mid, -1), up_rows(high, 1))
        for y, value in enumerate((jnp.maximum(mid, under), jnp.maximum(mid, over))):
            low_z = jnp.where(lane == 0, value, pltpu.roll(value, 1, 1))
            high_z = jnp.where(lane == LANES - 1, value, pltpu.roll(value, LANES - 1, 1))
            corners[x, y, 0] = jnp.maximum(value, low_z)
            corners[x, y, 1] = jnp.maximum(value, high_z)
    halves = [((1.0 - x) / 2.0, (1.0 + x) / 2.0) for x in NODES]
    for a in range(5):
        plane = {
            (y, z): mul(halves[a][0], corners[0, y, z]) + mul(halves[a][1], corners[1, y, z])
            for y in range(2)
            for z in range(2)
        }
        for b in range(5):
            low, high = (
                mul(halves[b][0], plane[0, z]) + mul(halves[b][1], plane[1, z]) for z in range(2)
            )
            for c in range(5):
                visc[25 * a + 5 * b + c] = mul(halves[c][0], low) + mul(halves[c][1], high)
    return corners


SHARE = 0.5 * LEFT * CORR_L
SHARE_FAR = float(np.sum(SHARE * (1.0 + NODES) / 2.0))
SHARE_NEAR = float(np.sum(SHARE * (1.0 - NODES) / 2.0))


def chord_send_kernel(gc, three, rkso, rse, visc, bco, bce, near):
    i, _ = row_ids()
    first_row = i == 0
    es, ec = even_span(), even_chord()
    corners = viscosity_into(
        visc, *((three[n],) + sided(es, rse[SPAN_N + n], rkso[n]) for n in range(3))
    )
    for n in range(4):
        y, z = n // 2, n % 2
        near[n] = SHARE_NEAR * jnp.where(first_row, -corners[0, y, z], corners[1, y, z])

    def far(n):
        return jnp.where(first_row, corners[1, n // 2, n % 2], corners[0, n // 2, n % 2])

    pack_chord(far, i, ec, bce, bco, CHORD_N, 4)

    def one(v, carry):
        def leaving(f):
            left, right = traces(even_odd([visc[p] * gc[v, p] for p in line_points(0, f)]))
            return jnp.where(first_row, left, right)

        pack_chord(leaving, i, ec, bce, bco, v * CHORD_V)
        return carry

    lax.fori_loop(0, NV, one, 0)


def span_flux_kernel(gs, visc, rse, rso, fs, bso, bse):
    _, j = row_ids()
    is_low = j == 0
    es = even_span()
    weights = span_weights(is_low)

    def one(v, carry):
        received = {}

        def leaving(f):
            m, q = f // 2, f % 2
            if m not in received:
                base = v * SPAN_V + m
                received[m] = sided(es, rse[base], rso[base])
            edge = open_span(received[m][0], received[m][1], q, is_low)
            values = []
            for k, p in enumerate(line_points(1, f)):
                value = visc[p] * (gs[v, p] + weights[k] * edge)
                fs[v, p] = value
                values.append(value)
            left, right = traces(even_odd(values))
            return jnp.where(is_low, left, right)

        pack_span(leaving, is_low, es, bse, bso, v * SPAN_V)
        return carry

    lax.fori_loop(0, NV, one, 0)


def factors_into(factor, far, near, behind_row):
    value = [
        jnp.where(behind_row, -SHARE_FAR, SHARE_FAR) * far[n] + near[n] for n in range(4)
    ]
    halves = [((1.0 - x) / 2.0, (1.0 + x) / 2.0) for x in NODES]
    for a in range(5):
        low, high = (
            mul(halves[a][0], value[z]) + mul(halves[a][1], value[2 + z]) for z in range(2)
        )
        for c in range(5):
            factor[5 * a + c] = mul(halves[c][0], low) + mul(halves[c][1], high)


def inner_kernel(state, visc, fs, gc, rce, rco, res, visc_out, total_ref, diff_ref, flux, sem):
    write = pltpu.make_async_copy(visc, visc_out, sem)
    write.start()
    i, j = row_ids()
    lane = lane_ids()
    is_low = j == 0
    sign_row = jnp.where(is_low, 1.0, -1.0)
    ec = even_chord()
    weights = chord_weights(i)

    def one(v, carry):
        received = {}

        def across(c):
            plane = {}
            for b in range(5):
                f = 5 * b + c
                m, q = f // 4, f % 4
                if m not in received:
                    at = v * CHORD_V + m
                    received[m] = sided(ec, rce[at], rco[at])
                edge = open_chord(*received[m], q, i)
                points = line_points(0, f)
                parts = even_odd(
                    [visc[p] * (gc[v, p] + weights[k] * edge) for k, p in enumerate(points)]
                )
                total, diff = neighbours_chord(*traces(parts), -1.0, i)
                plane.update(zip(points, slope(parts, total, diff)))
            for a in range(5):
                points = line_points(1, 5 * a + c)
                parts = even_odd([fs[v, p] for p in points])
                total, diff = neighbours_span(*traces(parts), is_low, sign_row)
                for p, value in zip(points, slope(parts, total, diff)):
                    res[v, p] = plane[p] + value

        for f in range(NF):
            ends = traces(even_odd([state[v, p] for p in line_points(2, f)]))
            total_ref[f], diff_ref[f] = neighbours_normal(*ends, 1.0, lane)
        across(0)
        across(1)
        for f in range(NF):
            points = line_points(2, f)
            parts = even_odd([state[v, p] for p in points])
            values = slope(parts, total_ref[f], diff_ref[f])
            values = [visc[p] * value for p, value in zip(points, values)]
            for p, value in zip(points, values):
                flux[p] = value
            ends = traces(even_odd(values))
            total_ref[NF + f], diff_ref[NF + f] = neighbours_normal(*ends, -1.0, lane)
        across(2)
        across(3)
        across(4)
        for f in range(NF):
            points = line_points(2, f)
            parts = even_odd([flux[p] for p in points])
            values = slope(parts, total_ref[NF + f], diff_ref[NF + f])
            for p, value in zip(points, values):
                res[v, p] = res[v, p] + value
        return carry

    lax.fori_loop(0, NV, one, 0)
    write.wait()


def close_chord_kernel(res, ce, co, rbce, rbco, near, out, factor):
    i, _ = row_ids()
    ec = even_chord()
    weights = chord_weights(i)
    far = sided(ec, rbce[CHORD_N], rbco[CHORD_N])
    factors_into(factor, [open_chord(*far, n, i) for n in range(4)], near, i == 0)

    def one(v, carry):
        for m in range(CHORD_V):
            at = v * CHORD_V + m
            received, own = sided(ec, rbce[at], rbco[at]), sided(ec, ce[at], co[at])
            for f in range(4 * m, min(4 * m + 4, NF)):
                q = f % 4
                edge = open_chord(*received, q, i) + factor[f] * open_chord(*own, q, i)
                for k, p in enumerate(line_points(0, f)):
                    out[v, p] = res[v, p] + weights[k] * edge
        return carry

    lax.fori_loop(0, NV, one, 0)


def close_span_kernel(res, rbse, rbso, final, edge, out, sems):
    _, j = row_ids()
    is_low = j == 0
    es = even_span()
    weights = span_weights(is_low)

    def send(v):
        return pltpu.make_async_copy(out.at[v], final.at[v], sems.at[v])

    def one(v, carry):
        for m in range(SPAN_V):
            first, second = rbse[v * SPAN_V + m], rbso[v * SPAN_V + m]
            behind, ahead = jnp.where(es, second, first), jnp.where(es, first, second)
            for f in range(2 * m, min(2 * m + 2, NF)):
                edge[f] = open_span(behind, ahead, f % 2, is_low)
        for f in range(NF):
            for k, p in enumerate(line_points(1, f)):
                out[v, p] = res[v, p] + weights[k] * edge[f]

        @pl.when(v > 0)
        def _():
            send(v - 1).start()

        return carry

    lax.fori_loop(0, NV, one, 0)
    send(NV - 1).start()
    for v in range(NV):
        send(v).wait()


def span_weights(is_low):
    return [jnp.where(is_low, float(0.5 * CORR_L[k]), float(0.5 * CORR_R[k])) for k in range(5)]


def chord_weights(i):
    first, last = chord_ends()
    low, high = jnp.logical_and(i == 0, ~first), jnp.logical_and(i == 3, ~last)
    return [
        jnp.where(low, float(0.5 * CORR_L[k]), jnp.where(high, float(0.5 * CORR_R[k]), 0.0))
        for k in range(5)
    ]


def held(*lead):
    return pltpu.VMEM(lead + (ROWS, LANES), jnp.float32)


def vec(*lead):
    return jax.ShapeDtypeStruct(lead + (ROWS, LANES), jnp.float32)


def call(kernel, outs, args, scratch=(), cycles=1000, far_in=(), far_out=(), grant=24 * 2**20):
    vmem, hbm = (pl.BlockSpec(memory_space=m) for m in (pltpu.VMEM, pltpu.HBM))
    total = sum(int(np.prod(x.shape)) for x in list(outs) + list(args)) * 4
    return pl.pallas_call(
        kernel,
        out_shape=outs,
        in_specs=[hbm if n in far_in else vmem for n in range(len(args))],
        out_specs=[hbm if n in far_out else vmem for n in range(len(outs))],
        scratch_shapes=list(scratch),
        compiler_params=pltpu.CompilerParams(vmem_limit_bytes=grant),
        cost_estimate=pl.CostEstimate(flops=cycles * 4096, bytes_accessed=total, transcendentals=0),
    )(*args)


def paired(n, odd, wraps):
    route = []
    for lower in range(odd, n, 2):
        upper = lower + 1
        if upper >= n:
            if not wraps:
                continue
            upper %= n
        route += [(lower, upper), (upper, lower)]
    return route


def shards(state):
    chords, spans = lax.axis_size("chord"), lax.axis_size("span")

    def span_swap(array, odd):
        return lax.ppermute(array, "span", paired(spans, odd, True))

    def chord_swap(array, odd):
        route = [
            (a * spans + c, b * spans + c) for a, b in paired(chords, odd, False) for c in range(spans)
        ]
        if odd:
            route += [
                (a * spans + c, a * spans + (c ^ 1)) for a in (0, chords - 1) for c in range(spans)
            ]
        return lax.ppermute(array, ("chord", "span"), route)

    dma = pltpu.SemaphoreType.DMA
    u = state.reshape(NV, 125, ROWS, LANES)
    (eps,) = call(
        sensor_kernel,
        [vec()],
        [pltpu.with_memory_space_constraint(u, pltpu.HBM)],
        [held(125), held(125), dma(())],
        far_in=(0,),
    )
    rkco = chord_swap(eps, 1)
    rkce = chord_swap(eps, 0)
    so, se = call(leave_span_kernel, [vec(SPAN_N), vec(SPAN_N)], [u])
    rso = span_swap(so, 1)
    three, se = call(three_kernel, [vec(3), vec(SPAN_N + 3)], [eps, rkce, rkco, se], cycles=100)
    rkso = span_swap(three, 1)
    co, ce = call(leave_chord_kernel, [vec(CHORD_N), vec(CHORD_N)], [u])
    rco = chord_swap(co, 1)
    rce = chord_swap(ce, 0)
    rse = span_swap(se, 0)
    gc, gs = call(gradient_kernel, [vec(NV, 125)] * 2, [u], cycles=4000)
    visc, bco, bce, near = call(
        chord_send_kernel,
        [vec(125), vec(CHORD_N + 1), vec(CHORD_N + 1), vec(4)],
        [gc, three, rkso, rse],
        cycles=2000,
    )
    rbco = chord_swap(bco, 1)
    fs, bso, bse = call(
        span_flux_kernel,
        [vec(NV, 125), vec(SPAN_N), vec(SPAN_N)],
        [gs, visc, rse, rso],
        cycles=2000,
    )
    rbso = span_swap(bso, 1)
    rbce = chord_swap(bce, 0)
    rbse = span_swap(bse, 0)
    res, visc_out = call(
        inner_kernel,
        [vec(NV, 125), vec(125)],
        [u, visc, fs, gc, rce, rco],
        [held(2 * NF), held(2 * NF), held(125), dma(())],
        cycles=8000,
        far_out=(1,),
    )
    (res,) = call(
        close_chord_kernel, [vec(NV, 125)], [res, ce, co, rbce, rbco, near], [held(NF)], cycles=1000
    )
    (out,) = call(
        close_span_kernel,
        [vec(NV, 125)],
        [res, rbse, rbso],
        [held(NF), held(NV, 125), dma((NV,))],
        cycles=2000,
        far_out=(0,),
    )
    return (out.reshape(state.shape), visc_out.reshape(state.shape[1:]))


def solution(mesh):
    in_specs = (P(None, None, "chord", "span", None),)
    out_specs = (P(None, None, "chord", "span", None), P(None, "chord", "span", None))

    return jax.shard_map(shards, mesh=mesh, in_specs=in_specs, out_specs=out_specs, check_vma=False)
```
